32 devices in a mesh: tm: 4 (over y, x), lat: 8 (over z, core).
Axes of the slice: x: 2, y: 2, z: 4, core: 2. Of those that a mesh axis runs over, the one named last changes fastest.
Arguments:
- sketch: bfloat16 [256, 3, 64, 1024], P('tm', None, 'lat'), may hold values from -6 to 6
- test_sketch: bfloat16 [256, 3, 64, 1024], P('tm', None, 'lat'), may hold values from -6 to 6
- checkpoints: bfloat16 [16, 3, 64, 1024], P('tm', None, 'lat'), may hold values from -2.5 to 2.5
- checkpoint_step: int32 [4], P('tm'), may hold values from 0 to 3
- station_row: int32 [4, 1024], P('tm', 'lat'), may hold values from 0 to 63, as said below
- station_column: int32 [4, 1024], P('tm', 'lat'), may hold values from 0 to 1023
- station_value: float32 [4, 1024], P('tm', 'lat'), may hold values from -6 to 6
Outputs:
- increment: float32 [4, 3, 64, 1024], P('tm', None, 'lat')
- reduced_adjoint: float32 [4, 64], P('tm')
- total_cost: float32 [], replicated
The draws below stay inside these ranges and needn't reach their ends.
Inputs may be any that keep to these rules, and one draw needn't show every extreme that they name: `station_row`: in each group's list, entries 128 * j to 128 * (j + 1) - 1 lie in latitude rows 8 * j to 8 * (j + 1) - 1.
All inputs are finite; a program needn't handle non-finite values.
Results may differ from the reference program's by a relative error of at most 0.0003.
Values may be sent and summed in bfloat16 or wider, within the bound.
A program may use at most 128 MiB of HBM per device.

```python
import math
import jax
import jax.numpy as jnp
from jax import lax

K = 64
ROWS = 8
NLON = 1024
STEPS = 4
NCK = 4
OBS_DEV = 128
NLAT = 64
NOBS = 1024
N_TM = 4


def draw_station_row(key, part):
    band = jnp.arange(NOBS, dtype=jnp.int32) // OBS_DEV
    offset = jax.random.randint(key, (N_TM, NOBS), 0, ROWS, dtype=jnp.int32)
    return band[None, :] * ROWS + offset


def plant(values, key, least, top_value):
    longest = values.shape.index(max(values.shape))
    spots = []
    for shift in (0, 1):
        where = [jax.random.randint(jax.random.fold_in(key, axis), (), 0, length) for axis, length in enumerate(values.shape)]
        where[longest] = (where[longest] + shift) % values.shape[longest]
        spots.append(tuple(where))
    return values.at[spots[0]].set(least).at[spots[1]].set(top_value)


def block_levels(own_key, shape, cuts, low, top_value):
    def one(position, parts):
        draws = jax.random.uniform(jax.random.fold_in(jax.random.fold_in(own_key, 6), position), (parts,), jnp.float32, low / len(cuts), top_value / len(cuts))
        return jnp.repeat(jnp.exp(draws), shape[position] // parts).reshape((-1,) + (1,) * (len(shape) - position - 1))

    factor_of = one(*cuts[0])
    for cut in cuts[1:]:
        factor_of = factor_of * one(*cut)
    return factor_of


def gaussian(key, extent, spread, reach, split=(), kind=jnp.bfloat16):
    loudness = block_levels(key, extent, split, -0.22, 0.18) if split else 1.0
    drawn = jax.random.normal(key, extent, jnp.float32) * spread * loudness
    return jnp.minimum(jnp.maximum(drawn, -reach), reach).astype(kind)


def setup_inputs(seed: int = 0) -> dict:
    arg_keys = jax.random.split(jax.random.key(seed), 8)
    return {
        "sketch": gaussian(arg_keys[0], (N_TM * K, 3, NLAT, NLON), 1.0, 6.0, ((0, 4), (2, 8))),
        "test_sketch": gaussian(arg_keys[1], (N_TM * K, 3, NLAT, NLON), 1.0, 6.0, ((0, 4), (2, 8))),
        "checkpoints": gaussian(arg_keys[2], (N_TM * NCK, 3, NLAT, NLON), 1.0, 2.5, ((0, 4), (2, 8))),
        "checkpoint_step": plant(jax.random.randint(arg_keys[3], (N_TM,), 0, NCK), jax.random.fold_in(arg_keys[3], 1), 0, NCK - 1).astype(jnp.int32),
        "station_row": draw_station_row(jax.random.fold_in(arg_keys[7], 71), 0),
        "station_column": plant(jax.random.randint(arg_keys[5], (N_TM, NOBS), 0, NLON), jax.random.fold_in(arg_keys[5], 1), 0, NLON - 1).astype(jnp.int32),
        "station_value": gaussian(arg_keys[6], (N_TM, NOBS), 1.0, 6.0, ((0, 4), (1, 8)), jnp.float32),
    }


wave_coef = 0.5
flow_coef = 0.4
coriolis_coef = 0.5
map_scale = 0.5

def coefficients(base_rows, first_row, total_rows):
    values = base_rows.astype(jnp.float32)
    depth = 1.0 + 0.25 * values[0]
    east_flow = 0.4 * values[1]
    north_flow = 0.4 * values[2]
    latitude = (first_row + jnp.arange(values.shape[1], dtype=jnp.int32)).astype(jnp.float32)
    coriolis = coriolis_coef * (2.0 * (latitude + 0.5) / total_rows - 1.0)
    return (depth, east_flow, north_flow, coriolis[:, None])

def advance(padded, depth, east_flow, north_flow, coriolis):
    height = padded[:, 0]
    eastward = padded[:, 1]
    northward = padded[:, 2]

    def along_lon(field):
        middle = field[:, 1:-1]
        return 0.5 * (jnp.roll(middle, -1, -1) - jnp.roll(middle, 1, -1))

    def along_lat(field):
        return 0.5 * (field[:, 2:] - field[:, :-2])
    centre_height = height[:, 1:-1]
    centre_east = eastward[:, 1:-1]
    centre_north = northward[:, 1:-1]
    new_east = centre_east + wave_coef * (coriolis * centre_north - along_lon(height)) - flow_coef * (east_flow * along_lon(eastward) + north_flow * along_lat(eastward))
    new_north = centre_north + wave_coef * (-coriolis * centre_east - along_lat(height)) - flow_coef * (east_flow * along_lon(northward) + north_flow * along_lat(northward))
    new_height = centre_height - wave_coef * depth * (along_lon(eastward) + along_lat(northward)) - flow_coef * (east_flow * along_lon(height) + north_flow * along_lat(height))
    return jnp.stack([new_height, new_east, new_north], 1)

def one_group(inputs):
    basis, tests, stored, chosen, rows, columns, values = inputs
    base = lax.dynamic_index_in_dim(stored, chosen, 0, keepdims=False)
    depth, east_flow, north_flow, coriolis = coefficients(base, 0, NLAT)
    state = basis.astype(jnp.float32)
    for step_index in range(STEPS):
        padded = jnp.pad(state, ((0, 0), (0, 0), (1, 1), (0, 0)))
        state = advance(padded, depth, east_flow, north_flow, coriolis)
    propagator = lax.dot_general(tests.reshape(K, -1).astype(jnp.float32), state.reshape(K, -1), (((1,), (1,)), ((), ())), precision=lax.Precision.HIGHEST, preferred_element_type=jnp.float32) * (map_scale / math.sqrt(K * 3 * NLAT * NLON))
    flat = (rows * NLON + columns).astype(jnp.int32)
    heights = basis[:, 0].reshape(K, -1)
    sampled = jnp.take(heights, flat, axis=1).astype(jnp.float32)
    innovation = jnp.take(base[0].reshape(-1), flat).astype(jnp.float32) - values
    weight = 1.0 + 2.0 * rows.astype(jnp.float32) / NLAT
    forcing = jnp.dot(sampled, weight * innovation, precision=lax.Precision.HIGHEST) / (2.0 * math.sqrt(NOBS))
    cost = jnp.sum(weight * innovation * innovation) / (2.0 * N_TM * NOBS)
    return (state, propagator, forcing, cost)

def reference(sketch, test_sketch, checkpoints, checkpoint_step, station_row, station_column, station_value):
    inputs = (sketch.reshape(N_TM, K, 3, NLAT, NLON), test_sketch.reshape(N_TM, K, 3, NLAT, NLON), checkpoints.reshape(N_TM, NCK, 3, NLAT, NLON), checkpoint_step, station_row, station_column, station_value)
    states, propagators, forcings, costs = lax.map(one_group, inputs)
    following = jnp.zeros((K,), jnp.float32)
    adjoints = [None] * N_TM
    for group in reversed(range(N_TM)):
        adjoint = jnp.dot(propagators[group].T, following, precision=lax.Precision.HIGHEST) + forcings[group]
        adjoints[group] = adjoint
        following = adjoint
    adjoint_stack = jnp.stack(adjoints)
    increment = jnp.einsum('gk,gkfrc->gfrc', adjoint_stack, states, precision=lax.Precision.HIGHEST) / math.sqrt(K)
    return (increment, adjoint_stack, jnp.sum(costs))
```

```python
import functools
import math

import jax
import jax.numpy as jnp
from jax import lax
from jax.experimental import pallas as pl
from jax.experimental.pallas import tpu as pltpu
from jax.sharding import PartitionSpec as P

STEPS = 4
LANES = 128

wave_coef = 0.5
flow_coef = 0.4
coriolis_coef = 0.5
map_scale = 0.5

MESH = pl.DeviceIdType.MESH


def dlat(field):
    count = field.shape[0]
    return pltpu.roll(field, count - 1, 0) - pltpu.roll(field, 1, 0)


def advance(state, coefs, turn, dlon):
    half = 0.5 * wave_coef
    dx_height, dx_east, dx_north = (dlon(values) for values in state)
    out = [], [], []
    for tile, (height, east, north) in enumerate(zip(*state)):
        depth, east_flow, north_flow = (values[tile] for values in coefs)
        dy_north = dlat(north)
        dy_height = dlat(height)
        out[0].append(
            height
            - depth * (dx_east[tile] + dy_north)
            - (east_flow * dx_height[tile] + north_flow * dy_height)
        )
        out[1].append(
            east
            + turn * north
            - half * dx_height[tile]
            - (east_flow * dx_east[tile] + north_flow * dlat(east))
        )
        out[2].append(
            north
            - turn * east
            - half * dy_height
            - (east_flow * dx_north[tile] + north_flow * dy_north)
        )
    return enumerate(out)


def advance_adjoint(state, coefs, turn, dlon):
    half = 0.5 * wave_coef
    heights, easts, norths = state
    depths, east_flows, north_flows = coefs
    cells = list(zip(heights, easts, norths, depths, east_flows, north_flows))
    dx = dlon([half * u + e * h for h, u, v, d, e, n in cells])
    yield 0, [h + x + dlat(half * v + n * h) for x, (h, u, v, d, e, n) in zip(dx, cells)]
    dx = dlon([d * h + e * u for h, u, v, d, e, n in cells])
    yield 1, [u - turn * v + x + dlat(n * u) for x, (h, u, v, d, e, n) in zip(dx, cells)]
    dx = dlon([e * v for h, u, v, d, e, n in cells])
    yield 2, [v + turn * u + x + dlat(d * h + n * v) for x, (h, u, v, d, e, n) in zip(dx, cells)]


def kernel(
    groups,
    bands,
    sketch_hbm,
    test_hbm,
    stored_hbm,
    chosen,
    row_hbm,
    column_hbm,
    value_hbm,
    increment,
    adjoint,
    total_cost,
    sketch,
    test,
    beyond,
    sketch_wide,
    test_wide,
    beyond_wide,
    stored,
    station_row,
    station_column,
    station_value,
    coef_ext,
    ext,
    spare,
    forced,
    forced_beyond,
    folded,
    spread,
    base_send,
    base_recv,
    field_send,
    field_recv,
    last_send,
    last_recv,
    message,
    later_in,
    own_in,
    cost_out,
    cost_in,
    cost_group_out,
    cost_group_in,
    cost_here,
    load_sem,
    beyond_ss,
    beyond_rs,
    base_ss,
    base_rs,
    field_ss,
    field_rs,
    last_ss,
    last_rs,
    later_ss,
    later_rs,
    own_ss,
    own_rs,
    cost_ss,
    cost_rs,
    cost_group_ss,
    cost_group_rs,
):
    rank, fields, rows, columns = sketch.shape
    halo = STEPS
    group = lax.axis_index("tm")
    band = lax.axis_index("lat")
    total_rows = rows * bands
    observed = station_row.shape[1] * bands
    tiles = columns // LANES

    loads = [
        pltpu.make_async_copy(source, target, load_sem.at[index])
        for index, (source, target) in enumerate(
            (
                (row_hbm, station_row),
                (column_hbm, station_column),
                (value_hbm, station_value),
                (stored_hbm, stored),
                (sketch_hbm.at[:, :1], sketch.at[:, :1]),
                (sketch_hbm.at[:, 1:], sketch.at[:, 1:]),
                (test_hbm, test),
            )
        )
    ]
    for load in loads[:6]:
        load.start()

    barrier = pltpu.get_barrier_semaphore()
    last_group = groups - 1

    def each(count, first, action):
        for index in range(first, count):
            action(index)

    def greet(place):
        pl.semaphore_signal(barrier, inc=1, device_id=place, device_id_type=MESH)

    @pl.when(group < last_group)
    def _():
        each(bands, 0, lambda index: greet({"tm": group + 1, "lat": index}))

    each(bands, 1, lambda offset: greet({"lat": lax.rem(band + offset, bands)}))

    for offset in range(2, groups):

        @pl.when(group + offset < groups)
        def _():
            greet({"tm": group + offset})

    for offset in range(1, groups):

        @pl.when(group - offset >= 0)
        def _():
            greet({"tm": group - offset})

    later = jnp.minimum(group, 1)
    greetings = bands - 1 + groups - 1 + (bands - 1) * later

    def remote(source, target, send_sem, recv_sem, where):
        return pltpu.make_async_remote_copy(
            src_ref=source,
            dst_ref=target,
            send_sem=send_sem,
            recv_sem=recv_sem,
            device_id=where,
            device_id_type=MESH,
        )

    below = {"lat": jnp.maximum(band - 1, 0)}
    above = {"lat": jnp.minimum(band + 1, bands - 1)}

    def halo_copies(send, recv, ss, rs, field):
        down = remote(
            send.at[0, field], recv.at[1, field], ss.at[0, field], rs.at[1, field], below
        )
        up = remote(send.at[1, field], recv.at[0, field], ss.at[1, field], rs.at[0, field], above)
        return down, up

    def halo_start(exchange, field):
        recv = exchange[1]
        down, up = halo_copies(*exchange, field)

        @pl.when(band > 0)
        def _():
            down.start()

        @pl.when(band == 0)
        def _():
            recv[0, field] = jnp.zeros(recv.shape[2:], recv.dtype)

        @pl.when(band < bands - 1)
        def _():
            up.start()

        @pl.when(band == bands - 1)
        def _():
            recv[1, field] = jnp.zeros(recv.shape[2:], recv.dtype)

    def halo_wait(exchange):
        @pl.when(band > 0)
        def _():
            for field in range(fields):
                halo_copies(*exchange, field)[1].wait_recv()

        @pl.when(band < bands - 1)
        def _():
            for field in range(fields):
                halo_copies(*exchange, field)[0].wait_recv()

    def halo_drain(exchange):
        @pl.when(band > 0)
        def _():
            for field in range(fields):
                halo_copies(*exchange, field)[0].wait_send()

        @pl.when(band < bands - 1)
        def _():
            for field in range(fields):
                halo_copies(*exchange, field)[1].wait_send()

    base_halo = (base_send, base_recv, base_ss, base_rs)
    field_halo = (field_send, field_recv, field_ss, field_rs)
    last_halo = (last_send, last_recv, last_ss, last_rs)

    for load in loads[:4]:
        load.wait()

    base_half = stored[chosen[0]]
    base = base_half.astype(jnp.float32)
    base_send[0] = base[:, :halo]
    base_send[1] = base[:, rows - halo :]

    cells = lax.broadcasted_iota(jnp.int32, (columns, station_column.shape[1]), 0)
    at_column = cells == station_column[...]
    local_row = station_row[...] - band * rows
    at_row = (
        lax.broadcasted_iota(jnp.int32, (rows, station_row.shape[1]), 0) == local_row
    )
    one_hot = at_column.astype(jnp.float32).astype(jnp.bfloat16)
    by_row = jnp.dot(
        base_half[0],
        one_hot,
        preferred_element_type=jnp.float32,
    )
    seen = jnp.sum(jnp.where(at_row, by_row, 0.0), axis=0, keepdims=True)
    innovation = seen - station_value[...]
    weight = 1.0 + 2.0 * station_row[...].astype(jnp.float32) / total_rows
    weighted = weight * innovation
    cost = jnp.sum(weighted * innovation, axis=1, keepdims=True) / (2.0 * groups * observed)
    cost_row = jnp.broadcast_to(cost, (1, LANES))
    cost_out[...] = cost_row
    source = jnp.where(at_row, weighted / (2.0 * math.sqrt(observed)), 0.0)
    parts = [source.astype(jnp.bfloat16).astype(jnp.float32)]
    parts.append((source - parts[0]).astype(jnp.bfloat16).astype(jnp.float32))
    parts.append(source - parts[0] - parts[1])
    parts.append(jnp.zeros_like(source))
    placed = lax.dot_general(
        jnp.concatenate(parts, axis=0).astype(jnp.bfloat16),
        one_hot,
        (((1,), (1,)), ((), ())),
        preferred_element_type=jnp.float32,
    )
    forced[0] = placed[:rows] + placed[rows : 2 * rows] + placed[2 * rows : 3 * rows]
    for field in range(1, fields):
        forced[field] = jnp.zeros((rows, columns), jnp.float32)

    eye = lax.broadcasted_iota(jnp.int32, (rank, LANES), 0) == lax.broadcasted_iota(
        jnp.int32, (rank, LANES), 1
    )

    def spread_row(row):
        column = jnp.sum(jnp.where(eye, row, 0.0), axis=1, keepdims=True)
        spread[...] = jnp.broadcast_to(column, (rank, LANES))

    block = 8

    def combined(basis, field):
        def some(index, total):
            for inner in range(2 * block):
                k = index * 2 * block + inner
                factor = jnp.broadcast_to(spread[pl.ds(k, 1), :], (rows, LANES))
                total = total + basis[k, field].astype(jnp.float32) * jnp.concatenate(
                    [factor] * tiles, axis=1
                )
            return total

        return lax.fori_loop(
            0, rank // (2 * block), some, jnp.zeros((rows, columns), jnp.float32)
        )

    def fold(pairs, kept):
        def some(index, carry):
            totals = [None] * block
            for basis, values in pairs:
                for field in range(kept):
                    value = values[field]
                    for inner in range(block):
                        product = basis[index * block + inner, field].astype(jnp.float32) * value
                        for tile in range(tiles):
                            term = product[:, tile * LANES : (tile + 1) * LANES]
                            before = totals[inner]
                            totals[inner] = term if before is None else before + term
            for inner in range(block):
                folded[pl.ds(index * block + inner, 1), :] = jnp.sum(
                    totals[inner], axis=0, keepdims=True
                )
            return carry

        lax.fori_loop(0, rank // block, some, 0)
        share = jnp.sum(folded[...], axis=1, keepdims=True)
        message[...] = jnp.sum(jnp.where(eye, share, 0.0), axis=0, keepdims=True)

    def widen(source, target):
        def some(index, carry):
            for inner in range(2):
                k = index * 2 + inner
                for field in range(fields):
                    target[k, field] = source[k, field].astype(jnp.float32)
            return carry

        lax.fori_loop(0, rank // 2, some, 0)

    loads[4].wait()

    @pl.when(group < last_group)
    def _():
        loads[6].start()
        loads[5].wait()

    @pl.when(group == last_group)
    def _():
        fold(((sketch, forced),), 1)

    pl.semaphore_wait(barrier, greetings)

    def later_copy(offset):
        other = lax.rem(band + offset, bands)
        return remote(
            message,
            later_in.at[band],
            later_ss.at[offset],
            later_rs.at[band],
            {"tm": jnp.maximum(group - 1, 0), "lat": other},
        )

    def own_copy(offset):
        other = lax.rem(band + offset, bands)
        return remote(
            message, own_in.at[band], own_ss.at[offset], own_rs.at[band], {"lat": other}
        )

    def own_arrival(offset):
        other = lax.rem(band + offset, bands)
        return remote(
            message, own_in.at[other], own_ss.at[offset], own_rs.at[other], {"lat": other}
        )

    def announce():
        @pl.when(group > 0)
        def _():
            each(bands, 0, lambda offset: later_copy(offset).start())

        each(bands, 1, lambda offset: own_copy(offset).start())
        own_in[band] = message[...]

    @pl.when(group == last_group)
    def _():
        announce()
        loads[5].wait()

    for field in range(fields):
        halo_start(base_halo, field)

    def cost_copy(offset):
        other = lax.rem(band + offset, bands)
        return remote(
            cost_out, cost_in.at[band], cost_ss.at[offset], cost_rs.at[band], {"lat": other}
        )

    def cost_arrival(offset):
        other = lax.rem(band + offset, bands)
        return remote(
            cost_out, cost_in.at[other], cost_ss.at[offset], cost_rs.at[other], {"lat": other}
        )

    each(bands, 1, lambda offset: cost_copy(offset).start())
    cost_in[band] = cost_row

    def cost_group_copy(offset):
        other = lax.rem(group + offset, groups)
        return remote(
            cost_group_out,
            cost_group_in.at[group],
            cost_group_ss.at[offset],
            cost_group_rs.at[group],
            {"tm": other},
        )

    def cost_group_arrival(offset):
        other = lax.rem(group + offset, groups)
        return remote(
            cost_group_out,
            cost_group_in.at[other],
            cost_group_ss.at[offset],
            cost_group_rs.at[other],
            {"tm": other},
        )

    def share_cost():
        each(bands, 1, lambda offset: cost_arrival(offset).wait_recv())
        group_cost = jnp.sum(cost_in[...], axis=0)
        cost_group_out[...] = group_cost
        each(groups, 1, lambda offset: cost_group_copy(offset).start())
        cost_group_in[group] = group_cost

    low, high = pl.ds(0, halo), pl.ds(halo, halo)
    top = pl.ds(rows - halo, halo)
    beyond_down = remote(
        sketch.at[:, :, low], beyond.at[:, :, low], beyond_ss.at[0], beyond_rs.at[1], below
    )
    beyond_up = remote(
        sketch.at[:, :, top], beyond.at[:, :, high], beyond_ss.at[1], beyond_rs.at[0], above
    )

    def clear(place):
        def one(k, carry):
            for field in range(fields):
                beyond[k, field, place] = jnp.zeros((halo, columns), beyond.dtype)
            return carry

        lax.fori_loop(0, rank, one, 0)

    @pl.when(group == 0)
    def _():
        @pl.when(band > 0)
        def _():
            beyond_down.start()

        @pl.when(band == 0)
        def _():
            clear(high)

        @pl.when(band < bands - 1)
        def _():
            beyond_up.start()

        @pl.when(band == bands - 1)
        def _():
            clear(low)

    @pl.when(group < last_group)
    def _():
        widen(sketch, sketch_wide)
        loads[6].wait()
        widen(test, test_wide)

    halo_wait(base_halo)
    scales = (0.5 * wave_coef * 0.25, 0.5 * flow_coef * 0.4, 0.5 * flow_coef * 0.4)
    starts = (0.5 * wave_coef, 0.0, 0.0)
    for field in range(fields):
        for place, part in (
            (pl.ds(0, rows), base[field]),
            (pl.ds(rows, halo), base_recv[1, field]),
            (pl.ds(rows + halo, halo), base_recv[0, field]),
        ):
            coef_ext[field, place] = starts[field] + scales[field] * part
    span = rows + 2 * halo
    inside = pl.ds(0, rows)
    after, before = pl.ds(rows, halo), pl.ds(rows + halo, halo)
    outside = pl.ds(rows, 2 * halo)

    def march(step_of, keep_outside):
        turned = lax.broadcasted_iota(jnp.int32, (span, LANES), 0)
        where = band * rows + jnp.where(turned < rows + halo, turned, turned - span)
        latitude = where.astype(jnp.float32)
        turn = wave_coef * coriolis_coef * (2.0 * (latitude + 0.5) / total_rows - 1.0)
        keep = jnp.where((where >= 0) & (where < total_rows), 1.0, 0.0)
        lane = lax.broadcasted_iota(jnp.int32, (span, LANES), 1)
        first, last = lane == 0, lane == LANES - 1

        def tiled(ref, field):
            return [ref[field, :, tile * LANES : (tile + 1) * LANES] for tile in range(tiles)]

        def dlon(values):
            ahead = [pltpu.roll(value, LANES - 1, 1) for value in values]
            behind = [pltpu.roll(value, 1, 1) for value in values]
            return [
                jnp.where(last, ahead[(tile + 1) % tiles], ahead[tile])
                - jnp.where(first, behind[tile - 1], behind[tile])
                for tile in range(tiles)
            ]

        coefs = [tiled(coef_ext, field) for field in range(fields)]
        source, target = ext, spare
        for step in range(STEPS):
            short = step == STEPS - 1 and not keep_outside
            state = [tiled(source, field) for field in range(fields)]
            for field, values in step_of(state, coefs, turn, dlon):
                for tile in range(tiles):
                    place = slice(tile * LANES, (tile + 1) * LANES)
                    value = values[tile] * keep
                    if short:
                        target[field, inside, place] = value[:rows]
                    else:
                        target[field, :, place] = value
            source, target = target, source

    def banded(basis, exchange):
        send, recv = exchange[:2]
        for field in range(fields):
            total = combined(basis, field)
            send[0, field] = total[:halo]
            send[1, field] = total[rows - halo :]
            halo_start(exchange, field)
            ext[field, inside] = total
        halo_wait(exchange)
        for field in range(fields):
            ext[field, before] = recv[0, field]
            ext[field, after] = recv[1, field]

    map_factor = map_scale / math.sqrt(rank * fields * total_rows * columns)

    def add_mapped():
        for field in range(fields):
            forced[field] = forced[field] + map_factor * ext[field, inside]

    @pl.when(group < last_group)
    def _():
        def arrive(offset):
            remote(
                message,
                later_in.at[offset],
                later_ss.at[offset],
                later_rs.at[offset],
                {"tm": group, "lat": offset},
            ).wait_recv()

        @pl.when(group == 0)
        def _():
            @pl.when(band > 0)
            def _():
                beyond_up.wait_recv()

            @pl.when(band < bands - 1)
            def _():
                beyond_down.wait_recv()

            widen(beyond, beyond_wide)

        @pl.when(group < last_group - 1)
        def _():
            share_cost()

        each(bands, 0, arrive)
        spread_row(jnp.sum(later_in[...], axis=0))

        @pl.when(group > 0)
        def _():
            banded(test_wide, field_halo)
            march(advance_adjoint, False)
            add_mapped()
            fold(((sketch_wide, forced),), fields)

        @pl.when(group == 0)
        def _():
            for field in range(fields):
                ext[field, inside] = combined(test_wide, field)
                ext[field, outside] = jnp.zeros((2 * halo, columns), jnp.float32)
            march(advance_adjoint, True)
            add_mapped()
            for field in range(fields):
                forced_beyond[field] = map_factor * ext[field, outside]

            fold(((sketch_wide, forced), (beyond_wide, forced_beyond)), fields)

        announce()

    @pl.when(group >= last_group - 1)
    def _():
        share_cost()

    each(groups, 1, lambda offset: cost_group_arrival(offset).wait_recv())
    cost_here[...] = jnp.sum(cost_group_in[...], axis=0)[:, :1]
    cost_store = pltpu.make_async_copy(cost_here, total_cost, load_sem.at[7])
    cost_store.start()

    each(bands, 1, lambda offset: own_arrival(offset).wait_recv())
    adjoint_row = jnp.sum(own_in[...], axis=0)
    adjoint[...] = adjoint_row[:, :rank]
    spread_row(adjoint_row)

    @pl.when(group > 0)
    def _():
        banded(sketch, last_halo)

    @pl.when(group == 0)
    def _():
        for field in range(fields):
            ext[field, inside] = combined(sketch_wide, field)
            ext[field, outside] = combined(beyond_wide, field)

    march(advance, False)
    for field in range(fields):
        increment[0, field] = ext[field, inside] / math.sqrt(rank)

    cost_store.wait()

    halo_drain(base_halo)
    each(bands, 1, lambda offset: cost_copy(offset).wait_send())
    each(bands, 1, lambda offset: own_copy(offset).wait_send())
    each(groups, 1, lambda offset: cost_group_copy(offset).wait_send())

    @pl.when(group > 0)
    def _():
        halo_drain(last_halo)
        each(bands, 0, lambda offset: later_copy(offset).wait_send())

    @pl.when((group > 0) & (group < last_group))
    def _():
        halo_drain(field_halo)

    @pl.when(group == 0)
    def _():
        @pl.when(band > 0)
        def _():
            beyond_down.wait_send()

        @pl.when(band < bands - 1)
        def _():
            beyond_up.wait_send()


def body(
    groups,
    bands,
    sketch,
    test_sketch,
    checkpoints,
    checkpoint_step,
    station_row,
    station_column,
    station_value,
):
    rank, fields, rows, columns = sketch.shape
    span = rows + 2 * STEPS
    f32 = jnp.float32

    def in_hbm(array):
        return pltpu.with_memory_space_constraint(array, pltpu.HBM)

    vmem = pl.BlockSpec(memory_space=pltpu.VMEM)
    hbm = pl.BlockSpec(memory_space=pltpu.HBM)
    edge = pltpu.VMEM((2, fields, STEPS, columns), f32)
    dma = pltpu.SemaphoreType.DMA
    increment, adjoint, cost = pl.pallas_call(
        functools.partial(kernel, groups, bands),
        out_shape=(
            jax.ShapeDtypeStruct((1, fields, rows, columns), f32),
            jax.ShapeDtypeStruct((1, rank), f32),
            jax.ShapeDtypeStruct((1, 1), f32),
        ),
        in_specs=[hbm, hbm, hbm, pl.BlockSpec(memory_space=pltpu.SMEM), hbm, hbm, hbm],
        out_specs=(vmem, vmem, hbm),
        scratch_shapes=[
            pltpu.VMEM(sketch.shape, sketch.dtype),
            pltpu.VMEM(test_sketch.shape, test_sketch.dtype),
            pltpu.VMEM((rank, fields, 2 * STEPS, columns), sketch.dtype),
            pltpu.VMEM(sketch.shape, f32),
            pltpu.VMEM(test_sketch.shape, f32),
            pltpu.VMEM((rank, fields, 2 * STEPS, columns), f32),
            pltpu.VMEM(checkpoints.shape, checkpoints.dtype),
            pltpu.VMEM(station_row.shape, station_row.dtype),
            pltpu.VMEM(station_column.shape, station_column.dtype),
            pltpu.VMEM(station_value.shape, station_value.dtype),
            pltpu.VMEM((fields, span, columns), f32),
            pltpu.VMEM((fields, span, columns), f32),
            pltpu.VMEM((fields, span, columns), f32),
            pltpu.VMEM((fields, rows, columns), f32),
            pltpu.VMEM((fields, 2 * STEPS, columns), f32),
            pltpu.VMEM((rank, LANES), f32),
            pltpu.VMEM((rank, LANES), f32),
            edge,
            edge,
            edge,
            edge,
            edge,
            edge,
            pltpu.VMEM((1, LANES), f32),
            pltpu.VMEM((bands, 1, LANES), f32),
            pltpu.VMEM((bands, 1, LANES), f32),
            pltpu.VMEM((1, LANES), f32),
            pltpu.VMEM((bands, 1, LANES), f32),
            pltpu.VMEM((1, LANES), f32),
            pltpu.VMEM((groups, 1, LANES), f32),
            pltpu.VMEM((1, 1), f32),
            dma((8,)),
            dma((2,)),
            dma((2,)),
            dma((2, fields)),
            dma((2, fields)),
            dma((2, fields)),
            dma((2, fields)),
            dma((2, fields)),
            dma((2, fields)),
            dma((bands,)),
            dma((bands,)),
            dma((bands,)),
            dma((bands,)),
            dma((bands,)),
            dma((bands,)),
            dma((groups,)),
            dma((groups,)),
        ],
        compiler_params=pltpu.CompilerParams(
            collective_id=0,
            has_side_effects=True,
            vmem_limit_bytes=48 * 1024 * 1024,
        ),
    )(
        in_hbm(sketch),
        in_hbm(test_sketch),
        in_hbm(checkpoints),
        checkpoint_step,
        in_hbm(station_row),
        in_hbm(station_column),
        in_hbm(station_value),
    )
    return increment, adjoint, cost[0, 0]


def solution(mesh):
    placed = (
        P("tm", None, "lat", None),
        P("tm", None, "lat", None),
        P("tm", None, "lat", None),
        P("tm"),
        P("tm", "lat"),
        P("tm", "lat"),
        P("tm", "lat"),
    )
    return jax.shard_map(
        functools.partial(body, mesh.shape["tm"], mesh.shape["lat"]),
        mesh=mesh,
        in_specs=placed,
        out_specs=(P("tm", None, "lat", None), P("tm", None), P()),
        check_vma=False,
    )
```

```python
import functools
import math

import jax
import jax.numpy as jnp
from jax import lax
from jax.experimental import pallas as pl
from jax.experimental.pallas import tpu as pltpu
from jax.sharding import PartitionSpec as P

STEPS = 4
LANES = 128

wave_coef = 0.5
flow_coef = 0.4
coriolis_coef = 0.5
map_scale = 0.5

MESH = pl.DeviceIdType.MESH


def dlat(field):
    count = field.shape[0]
    return pltpu.roll(field, count - 1, 0) - pltpu.roll(field, 1, 0)


def advance(state, coefs, turn, dlon):
    half = 0.5 * wave_coef
    dx_height, dx_east, dx_north = (dlon(values) for values in state)
    out = [], [], []
    for tile, (height, east, north) in enumerate(zip(*state)):
        depth, east_flow, north_flow = (values[tile] for values in coefs)
        dy_north = dlat(north)
        dy_height = dlat(height)
        out[0].append(
            height
            - depth * (dx_east[tile] + dy_north)
            - (east_flow * dx_height[tile] + north_flow * dy_height)
        )
        out[1].append(
            east
            + turn * north
            - half * dx_height[tile]
            - (east_flow * dx_east[tile] + north_flow * dlat(east))
        )
        out[2].append(
            north
            - turn * east
            - half * dy_height
            - (east_flow * dx_north[tile] + north_flow * dy_north)
        )
    return enumerate(out)


def advance_adjoint(state, coefs, turn, dlon):
    half = 0.5 * wave_coef
    heights, easts, norths = state
    depths, east_flows, north_flows = coefs
    cells = list(zip(heights, easts, norths, depths, east_flows, north_flows))
    dx = dlon([half * u + e * h for h, u, v, d, e, n in cells])
    yield 0, [h + x + dlat(half * v + n * h) for x, (h, u, v, d, e, n) in zip(dx, cells)]
    dx = dlon([d * h + e * u for h, u, v, d, e, n in cells])
    yield 1, [u - turn * v + x + dlat(n * u) for x, (h, u, v, d, e, n) in zip(dx, cells)]
    dx = dlon([e * v for h, u, v, d, e, n in cells])
    yield 2, [v + turn * u + x + dlat(d * h + n * v) for x, (h, u, v, d, e, n) in zip(dx, cells)]


def kernel(
    groups,
    bands,
    sketch_hbm,
    test_hbm,
    stored_hbm,
    chosen,
    row_hbm,
    column_hbm,
    value_hbm,
    increment,
    adjoint,
    total_cost,
    sketch,
    test,
    beyond,
    sketch_wide,
    test_wide,
    beyond_wide,
    stored,
    station_row,
    station_column,
    station_value,
    coef_ext,
    ext,
    spare,
    forced,
    forced_beyond,
    folded,
    spread,
    base_send,
    base_recv,
    field_send,
    field_recv,
    last_send,
    last_recv,
    message,
    later_in,
    own_in,
    cost_out,
    cost_in,
    cost_group_out,
    cost_group_in,
    cost_here,
    load_sem,
    beyond_ss,
    beyond_rs,
    base_ss,
    base_rs,
    field_ss,
    field_rs,
    last_ss,
    last_rs,
    later_ss,
    later_rs,
    own_ss,
    own_rs,
    cost_ss,
    cost_rs,
    cost_group_ss,
    cost_group_rs,
):
    rank, fields, rows, columns = sketch.shape
    halo = STEPS
    group = lax.axis_index("tm")
    band = lax.axis_index("lat")
    total_rows = rows * bands
    observed = station_row.shape[1] * bands
    tiles = columns // LANES

    loads = [
        pltpu.make_async_copy(source, target, load_sem.at[index])
        for index, (source, target) in enumerate(
            (
                (row_hbm, station_row),
                (column_hbm, station_column),
                (value_hbm, station_value),
                (stored_hbm, stored),
                (sketch_hbm.at[:, :1], sketch.at[:, :1]),
                (sketch_hbm.at[:, 1:], sketch.at[:, 1:]),
                (test_hbm, test),
            )
        )
    ]
    for load in loads[:6]:
        load.start()

    barrier = pltpu.get_barrier_semaphore()
    last_group = groups - 1

    def each(count, first, action):
        for index in range(first, count):
            action(index)

    def greet(place):
        pl.semaphore_signal(barrier, inc=1, device_id=place, device_id_type=MESH)

    @pl.when(group < last_group)
    def _():
        each(bands, 0, lambda index: greet({"tm": group + 1, "lat": index}))

    each(bands, 1, lambda offset: greet({"lat": lax.rem(band + offset, bands)}))

    for offset in range(2, groups):

        @pl.when(group + offset < groups)
        def _():
            greet({"tm": group + offset})

    for offset in range(1, groups):

        @pl.when(group - offset >= 0)
        def _():
            greet({"tm": group - offset})

    later = jnp.minimum(group, 1)
    greetings = bands - 1 + groups - 1 + (bands - 1) * later

    def remote(source, target, send_sem, recv_sem, where):
        return pltpu.make_async_remote_copy(
            src_ref=source,
            dst_ref=target,
            send_sem=send_sem,
            recv_sem=recv_sem,
            device_id=where,
            device_id_type=MESH,
        )

    below = {"lat": jnp.maximum(band - 1, 0)}
    above = {"lat": jnp.minimum(band + 1, bands - 1)}

    def halo_copies(send, recv, ss, rs, field):
        down = remote(send.at[0, field], recv.at[1, field], ss.at[0], rs.at[0], below)
        up = remote(send.at[1, field], recv.at[0, field], ss.at[0], rs.at[0], above)
        return down, up

    def halo_start(exchange, field):
        recv = exchange[1]
        down, up = halo_copies(*exchange, field)

        @pl.when(band > 0)
        def _():
            down.start()

        @pl.when(band == 0)
        def _():
            recv[0, field] = jnp.zeros(recv.shape[2:], recv.dtype)

        @pl.when(band < bands - 1)
        def _():
            up.start()

        @pl.when(band == bands - 1)
        def _():
            recv[1, field] = jnp.zeros(recv.shape[2:], recv.dtype)

    def both_or_one(action):
        @pl.when((band > 0) & (band < bands - 1))
        def _():
            action(slice(None))

        @pl.when(band == 0)
        def _():
            action(1)

        @pl.when(band == bands - 1)
        def _():
            action(0)

    def halo_wait(exchange):
        _, recv, ss, rs = exchange

        def one(place):
            remote(recv.at[place], recv.at[place], ss.at[0], rs.at[0], above).wait_recv()

        both_or_one(one)

    def halo_drain(exchange):
        send, _, ss, rs = exchange

        def one(place):
            remote(send.at[place], send.at[place], ss.at[0], rs.at[0], above).wait_send()

        both_or_one(one)

    base_halo = (base_send, base_recv, base_ss, base_rs)
    field_halo = (field_send, field_recv, field_ss, field_rs)
    last_halo = (last_send, last_recv, last_ss, last_rs)

    for load in loads[:4]:
        load.wait()

    base_half = stored[chosen[0]]
    base = base_half.astype(jnp.float32)
    base_send[0] = base[:, :halo]
    base_send[1] = base[:, rows - halo :]

    cells = lax.broadcasted_iota(jnp.int32, (columns, station_column.shape[1]), 0)
    at_column = cells == station_column[...]
    local_row = station_row[...] - band * rows
    at_row = (
        lax.broadcasted_iota(jnp.int32, (rows, station_row.shape[1]), 0) == local_row
    )
    one_hot = at_column.astype(jnp.float32).astype(jnp.bfloat16)
    by_row = jnp.dot(
        base_half[0],
        one_hot,
        preferred_element_type=jnp.float32,
    )
    seen = jnp.sum(jnp.where(at_row, by_row, 0.0), axis=0, keepdims=True)
    innovation = seen - station_value[...]
    weight = 1.0 + 2.0 * station_row[...].astype(jnp.float32) / total_rows
    weighted = weight * innovation
    cost = jnp.sum(weighted * innovation, axis=1, keepdims=True) / (2.0 * groups * observed)
    cost_row = jnp.broadcast_to(cost, (1, LANES))
    cost_out[...] = cost_row
    source = jnp.where(at_row, weighted / (2.0 * math.sqrt(observed)), 0.0)
    parts = [source.astype(jnp.bfloat16).astype(jnp.float32)]
    parts.append((source - parts[0]).astype(jnp.bfloat16).astype(jnp.float32))
    parts.append(source - parts[0] - parts[1])
    parts.append(jnp.zeros_like(source))
    placed = lax.dot_general(
        jnp.concatenate(parts, axis=0).astype(jnp.bfloat16),
        one_hot,
        (((1,), (1,)), ((), ())),
        preferred_element_type=jnp.float32,
    )
    forced[0] = placed[:rows] + placed[rows : 2 * rows] + placed[2 * rows : 3 * rows]
    for field in range(1, fields):
        forced[field] = jnp.zeros((rows, columns), jnp.float32)

    eye = lax.broadcasted_iota(jnp.int32, (rank, LANES), 0) == lax.broadcasted_iota(
        jnp.int32, (rank, LANES), 1
    )

    def spread_row(row):
        column = jnp.sum(jnp.where(eye, row, 0.0), axis=1, keepdims=True)
        spread[...] = jnp.broadcast_to(column, (rank, LANES))

    block = 8

    def combined(basis, field):
        def some(index, total):
            for inner in range(2 * block):
                k = index * 2 * block + inner
                factor = jnp.broadcast_to(spread[pl.ds(k, 1), :], (rows, LANES))
                total = total + basis[k, field].astype(jnp.float32) * jnp.concatenate(
                    [factor] * tiles, axis=1
                )
            return total

        return lax.fori_loop(
            0, rank // (2 * block), some, jnp.zeros((rows, columns), jnp.float32)
        )

    def fold(pairs, kept):
        def some(index, carry):
            totals = [None] * block
            for basis, values in pairs:
                for field in range(kept):
                    value = values[field]
                    for inner in range(block):
                        product = basis[index * block + inner, field].astype(jnp.float32) * value
                        for tile in range(tiles):
                            term = product[:, tile * LANES : (tile + 1) * LANES]
                            before = totals[inner]
                            totals[inner] = term if before is None else before + term
            for inner in range(block):
                folded[pl.ds(index * block + inner, 1), :] = jnp.sum(
                    totals[inner], axis=0, keepdims=True
                )
            return carry

        lax.fori_loop(0, rank // block, some, 0)
        share = jnp.sum(folded[...], axis=1, keepdims=True)
        message[...] = jnp.sum(jnp.where(eye, share, 0.0), axis=0, keepdims=True)

    def widen(source, target, start, stop):
        def some(index, carry):
            for inner in range(2):
                k = index * 2 + inner
                for field in range(fields):
                    target[k, field] = source[k, field].astype(jnp.float32)
            return carry

        lax.fori_loop(start // 2, stop // 2, some, 0)

    loads[4].wait()

    @pl.when(group < last_group)
    def _():
        loads[6].start()
        loads[5].wait()

    @pl.when(group == last_group)
    def _():
        fold(((sketch, forced),), 1)

    pl.semaphore_wait(barrier, greetings)

    def later_copy(offset):
        other = lax.rem(band + offset, bands)
        return remote(
            message,
            later_in.at[band],
            later_ss.at[0],
            later_rs.at[0],
            {"tm": jnp.maximum(group - 1, 0), "lat": other},
        )

    def own_copy(offset):
        other = lax.rem(band + offset, bands)
        return remote(
            message, own_in.at[band], own_ss.at[0], own_rs.at[0], {"lat": other}
        )

    def group_end(buffer, count, ss, rs):
        place = buffer.at[pl.ds(0, count)]
        return remote(place, place, ss.at[0], rs.at[0], {"lat": lax.rem(band + 1, bands)})

    def announce():
        @pl.when(group > 0)
        def _():
            each(bands, 0, lambda offset: later_copy(offset).start())

        each(bands, 1, lambda offset: own_copy(offset).start())
        own_in[band] = message[...]

    @pl.when(group == last_group)
    def _():
        announce()
        loads[5].wait()

    for field in range(fields):
        halo_start(base_halo, field)

    def cost_copy(offset):
        other = lax.rem(band + offset, bands)
        return remote(
            cost_out, cost_in.at[band], cost_ss.at[0], cost_rs.at[0], {"lat": other}
        )

    each(bands, 1, lambda offset: cost_copy(offset).start())
    cost_in[band] = cost_row

    def cost_group_copy(offset):
        other = lax.rem(group + offset, groups)
        return remote(
            cost_group_out,
            cost_group_in.at[group],
            cost_group_ss.at[0],
            cost_group_rs.at[0],
            {"tm": other},
        )

    def share_cost():
        group_end(cost_in, bands - 1, cost_ss, cost_rs).wait_recv()
        group_cost = jnp.sum(cost_in[...], axis=0)
        cost_group_out[...] = group_cost
        each(groups, 1, lambda offset: cost_group_copy(offset).start())
        cost_group_in[group] = group_cost

    low, high = pl.ds(0, halo), pl.ds(halo, halo)
    top = pl.ds(rows - halo, halo)
    early = rank * 3 // 4
    lots = (pl.ds(0, early), pl.ds(early, rank - early))

    def beyond_copies(lot):
        columns_of = lots[lot]
        return (
            remote(
                sketch.at[columns_of, :, low],
                beyond.at[columns_of, :, low],
                beyond_ss.at[lot],
                beyond_rs.at[lot],
                below,
            ),
            remote(
                sketch.at[columns_of, :, top],
                beyond.at[columns_of, :, high],
                beyond_ss.at[lot],
                beyond_rs.at[lot],
                above,
            ),
        )

    def beyond_end(lot):
        ends = {}

        def one(place):
            rows_of = pl.ds(0, 2 * halo) if isinstance(place, slice) else low
            part = beyond.at[lots[lot], :, rows_of]
            ends[0] = remote(part, part, beyond_ss.at[lot], beyond_rs.at[lot], above)

        return one, ends

    def beyond_wait(lot, sent):
        one, ends = beyond_end(lot)

        def wait(place):
            one(place)
            ends[0].wait_send() if sent else ends[0].wait_recv()

        both_or_one(wait)

    def clear(place):
        def one(k, carry):
            for field in range(fields):
                beyond[k, field, place] = jnp.zeros((halo, columns), beyond.dtype)
            return carry

        lax.fori_loop(0, rank, one, 0)

    @pl.when(group == 0)
    def _():
        @pl.when(band > 0)
        def _():
            for lot in range(2):
                beyond_copies(lot)[0].start()

        @pl.when(band == 0)
        def _():
            clear(high)

        @pl.when(band < bands - 1)
        def _():
            for lot in range(2):
                beyond_copies(lot)[1].start()

        @pl.when(band == bands - 1)
        def _():
            clear(low)

    @pl.when(group < last_group)
    def _():
        widen(sketch, sketch_wide, 0, rank)
        loads[6].wait()
        widen(test, test_wide, 0, rank)

    halo_wait(base_halo)
    scales = (0.5 * wave_coef * 0.25, 0.5 * flow_coef * 0.4, 0.5 * flow_coef * 0.4)
    starts = (0.5 * wave_coef, 0.0, 0.0)
    for field in range(fields):
        for place, part in (
            (pl.ds(0, rows), base[field]),
            (pl.ds(rows, halo), base_recv[1, field]),
            (pl.ds(rows + halo, halo), base_recv[0, field]),
        ):
            coef_ext[field, place] = starts[field] + scales[field] * part
    span = rows + 2 * halo
    inside = pl.ds(0, rows)
    after, before = pl.ds(rows, halo), pl.ds(rows + halo, halo)
    outside = pl.ds(rows, 2 * halo)

    def march(step_of, keep_outside):
        turned = lax.broadcasted_iota(jnp.int32, (span, LANES), 0)
        where = band * rows + jnp.where(turned < rows + halo, turned, turned - span)
        latitude = where.astype(jnp.float32)
        turn = wave_coef * coriolis_coef * (2.0 * (latitude + 0.5) / total_rows - 1.0)
        keep = jnp.where((where >= 0) & (where < total_rows), 1.0, 0.0)
        lane = lax.broadcasted_iota(jnp.int32, (span, LANES), 1)
        first, last = lane == 0, lane == LANES - 1

        def tiled(ref, field):
            return [ref[field, :, tile * LANES : (tile + 1) * LANES] for tile in range(tiles)]

        def dlon(values):
            ahead = [pltpu.roll(value, LANES - 1, 1) for value in values]
            behind = [pltpu.roll(value, 1, 1) for value in values]
            return [
                jnp.where(last, ahead[(tile + 1) % tiles], ahead[tile])
                - jnp.where(first, behind[tile - 1], behind[tile])
                for tile in range(tiles)
            ]

        coefs = [tiled(coef_ext, field) for field in range(fields)]
        source, target = ext, spare
        for step in range(STEPS):
            short = step == STEPS - 1 and not keep_outside
            state = [tiled(source, field) for field in range(fields)]
            for field, values in step_of(state, coefs, turn, dlon):
                for tile in range(tiles):
                    place = slice(tile * LANES, (tile + 1) * LANES)
                    value = values[tile] * keep
                    if short:
                        target[field, inside, place] = value[:rows]
                    else:
                        target[field, :, place] = value
            source, target = target, source

    def banded(basis, exchange):
        send, recv = exchange[:2]
        for field in range(fields):
            total = combined(basis, field)
            send[0, field] = total[:halo]
            send[1, field] = total[rows - halo :]
            halo_start(exchange, field)
            ext[field, inside] = total
        halo_wait(exchange)
        for field in range(fields):
            ext[field, before] = recv[0, field]
            ext[field, after] = recv[1, field]

    map_factor = map_scale / math.sqrt(rank * fields * total_rows * columns)

    def add_mapped():
        for field in range(fields):
            forced[field] = forced[field] + map_factor * ext[field, inside]

    @pl.when(group < last_group)
    def _():
        @pl.when(group < last_group - 1)
        def _():
            share_cost()

        @pl.when(group == 0)
        def _():
            beyond_wait(0, False)
            widen(beyond, beyond_wide, 0, early)
            beyond_wait(1, False)
            widen(beyond, beyond_wide, early, rank)

        group_end(later_in, bands, later_ss, later_rs).wait_recv()
        spread_row(jnp.sum(later_in[...], axis=0))

        @pl.when(group > 0)
        def _():
            banded(test_wide, field_halo)
            march(advance_adjoint, False)
            add_mapped()
            fold(((sketch_wide, forced),), fields)

        @pl.when(group == 0)
        def _():
            for field in range(fields):
                ext[field, inside] = combined(test_wide, field)
                ext[field, outside] = jnp.zeros((2 * halo, columns), jnp.float32)
            march(advance_adjoint, True)
            add_mapped()
            for field in range(fields):
                forced_beyond[field] = map_factor * ext[field, outside]

            fold(((sketch_wide, forced), (beyond_wide, forced_beyond)), fields)

        announce()

    @pl.when(group >= last_group - 1)
    def _():
        share_cost()

    group_end(cost_group_in, groups - 1, cost_group_ss, cost_group_rs).wait_recv()
    cost_here[...] = jnp.sum(cost_group_in[...], axis=0)[:, :1]
    cost_store = pltpu.make_async_copy(cost_here, total_cost, load_sem.at[7])
    cost_store.start()

    group_end(own_in, bands - 1, own_ss, own_rs).wait_recv()
    adjoint_row = jnp.sum(own_in[...], axis=0)
    adjoint[...] = adjoint_row[:, :rank]
    spread_row(adjoint_row)

    @pl.when(group > 0)
    def _():
        banded(sketch, last_halo)

    @pl.when(group == 0)
    def _():
        for field in range(fields):
            ext[field, inside] = combined(sketch_wide, field)
            ext[field, outside] = combined(beyond_wide, field)

    march(advance, False)
    for field in range(fields):
        increment[0, field] = ext[field, inside] / math.sqrt(rank)

    cost_store.wait()

    halo_drain(base_halo)
    group_end(cost_in, bands - 1, cost_ss, cost_rs).wait_send()
    group_end(own_in, bands - 1, own_ss, own_rs).wait_send()
    group_end(cost_group_in, groups - 1, cost_group_ss, cost_group_rs).wait_send()

    @pl.when(group > 0)
    def _():
        halo_drain(last_halo)
        group_end(later_in, bands, later_ss, later_rs).wait_send()

    @pl.when((group > 0) & (group < last_group))
    def _():
        halo_drain(field_halo)

    @pl.when(group == 0)
    def _():
        for lot in range(2):
            beyond_wait(lot, True)


def body(
    groups,
    bands,
    sketch,
    test_sketch,
    checkpoints,
    checkpoint_step,
    station_row,
    station_column,
    station_value,
):
    rank, fields, rows, columns = sketch.shape
    span = rows + 2 * STEPS
    f32 = jnp.float32

    def in_hbm(array):
        return pltpu.with_memory_space_constraint(array, pltpu.HBM)

    vmem = pl.BlockSpec(memory_space=pltpu.VMEM)
    hbm = pl.BlockSpec(memory_space=pltpu.HBM)
    edge = pltpu.VMEM((2, fields, STEPS, columns), f32)
    dma = pltpu.SemaphoreType.DMA
    increment, adjoint, cost = pl.pallas_call(
        functools.partial(kernel, groups, bands),
        out_shape=(
            jax.ShapeDtypeStruct((1, fields, rows, columns), f32),
            jax.ShapeDtypeStruct((1, rank), f32),
            jax.ShapeDtypeStruct((1, 1), f32),
        ),
        in_specs=[hbm, hbm, hbm, pl.BlockSpec(memory_space=pltpu.SMEM), hbm, hbm, hbm],
        out_specs=(vmem, vmem, hbm),
        scratch_shapes=[
            pltpu.VMEM(sketch.shape, sketch.dtype),
            pltpu.VMEM(test_sketch.shape, test_sketch.dtype),
            pltpu.VMEM((rank, fields, 2 * STEPS, columns), sketch.dtype),
            pltpu.VMEM(sketch.shape, f32),
            pltpu.VMEM(test_sketch.shape, f32),
            pltpu.VMEM((rank, fields, 2 * STEPS, columns), f32),
            pltpu.VMEM(checkpoints.shape, checkpoints.dtype),
            pltpu.VMEM(station_row.shape, station_row.dtype),
            pltpu.VMEM(station_column.shape, station_column.dtype),
            pltpu.VMEM(station_value.shape, station_value.dtype),
            pltpu.VMEM((fields, span, columns), f32),
            pltpu.VMEM((fields, span, columns), f32),
            pltpu.VMEM((fields, span, columns), f32),
            pltpu.VMEM((fields, rows, columns), f32),
            pltpu.VMEM((fields, 2 * STEPS, columns), f32),
            pltpu.VMEM((rank, LANES), f32),
            pltpu.VMEM((rank, LANES), f32),
            edge,
            edge,
            edge,
            edge,
            edge,
            edge,
            pltpu.VMEM((1, LANES), f32),
            pltpu.VMEM((bands, 1, LANES), f32),
            pltpu.VMEM((bands, 1, LANES), f32),
            pltpu.VMEM((1, LANES), f32),
            pltpu.VMEM((bands, 1, LANES), f32),
            pltpu.VMEM((1, LANES), f32),
            pltpu.VMEM((groups, 1, LANES), f32),
            pltpu.VMEM((1, 1), f32),
            dma((8,)),
            dma((2,)),
            dma((2,)),
            dma((1,)),
            dma((1,)),
            dma((1,)),
            dma((1,)),
            dma((1,)),
            dma((1,)),
            dma((1,)),
            dma((1,)),
            dma((1,)),
            dma((1,)),
            dma((1,)),
            dma((1,)),
            dma((1,)),
            dma((1,)),
        ],
        compiler_params=pltpu.CompilerParams(
            collective_id=0,
            has_side_effects=True,
            vmem_limit_bytes=48 * 1024 * 1024,
        ),
    )(
        in_hbm(sketch),
        in_hbm(test_sketch),
        in_hbm(checkpoints),
        checkpoint_step,
        in_hbm(station_row),
        in_hbm(station_column),
        in_hbm(station_value),
    )
    return increment, adjoint, cost[0, 0]


def solution(mesh):
    placed = (
        P("tm", None, "lat", None),
        P("tm", None, "lat", None),
        P("tm", None, "lat", None),
        P("tm"),
        P("tm", "lat"),
        P("tm", "lat"),
        P("tm", "lat"),
    )
    return jax.shard_map(
        functools.partial(body, mesh.shape["tm"], mesh.shape["lat"]),
        mesh=mesh,
        in_specs=placed,
        out_specs=(P("tm", None, "lat", None), P("tm", None), P()),
        check_vma=False,
    )
```

```python
import functools
import math

import jax
import jax.numpy as jnp
from jax import lax
from jax.experimental import pallas as pl
from jax.experimental.pallas import tpu as pltpu
from jax.sharding import PartitionSpec as P

STEPS = 4
LANES = 128

wave_coef = 0.5
flow_coef = 0.4
coriolis_coef = 0.5
map_scale = 0.5

MESH = pl.DeviceIdType.MESH


def dlat(field):
    count = field.shape[0]
    return pltpu.roll(field, count - 1, 0) - pltpu.roll(field, 1, 0)


def advance(state, coefs, turn, dlon):
    half = 0.5 * wave_coef
    dx_height, dx_east, dx_north = (dlon(values) for values in state)
    out = [], [], []
    for tile, (height, east, north) in enumerate(zip(*state)):
        depth, east_flow, north_flow = (values[tile] for values in coefs)
        dy_north = dlat(north)
        dy_height = dlat(height)
        out[0].append(
            height
            - depth * (dx_east[tile] + dy_north)
            - (east_flow * dx_height[tile] + north_flow * dy_height)
        )
        out[1].append(
            east
            + turn * north
            - half * dx_height[tile]
            - (east_flow * dx_east[tile] + north_flow * dlat(east))
        )
        out[2].append(
            north
            - turn * east
            - half * dy_height
            - (east_flow * dx_north[tile] + north_flow * dy_north)
        )
    return enumerate(out)


def advance_adjoint(state, coefs, turn, dlon):
    half = 0.5 * wave_coef
    heights, easts, norths = state
    depths, east_flows, north_flows = coefs
    cells = list(zip(heights, easts, norths, depths, east_flows, north_flows))
    dx = dlon([half * u + e * h for h, u, v, d, e, n in cells])
    yield 0, [h + x + dlat(half * v + n * h) for x, (h, u, v, d, e, n) in zip(dx, cells)]
    dx = dlon([d * h + e * u for h, u, v, d, e, n in cells])
    yield 1, [u - turn * v + x + dlat(n * u) for x, (h, u, v, d, e, n) in zip(dx, cells)]
    dx = dlon([e * v for h, u, v, d, e, n in cells])
    yield 2, [v + turn * u + x + dlat(d * h + n * v) for x, (h, u, v, d, e, n) in zip(dx, cells)]


def kernel(
    groups,
    bands,
    sketch_hbm,
    test_hbm,
    stored_hbm,
    chosen,
    row_hbm,
    column_hbm,
    value_hbm,
    increment,
    adjoint,
    sketch,
    test,
    beyond,
    sketch_wide,
    test_wide,
    beyond_wide,
    stored,
    station_row,
    station_column,
    station_value,
    coef_ext,
    ext,
    spare,
    forced,
    forced_beyond,
    folded,
    spread,
    base_send,
    base_recv,
    field_send,
    field_recv,
    last_send,
    last_recv,
    message,
    later_in,
    own_in,
    cost_out,
    cost_in,
    cost_group_out,
    cost_group_in,
    cost_here,
    load_sem,
    beyond_ss,
    beyond_rs,
    base_ss,
    base_rs,
    field_ss,
    field_rs,
    last_ss,
    last_rs,
    later_ss,
    later_rs,
    own_ss,
    own_rs,
    cost_ss,
    cost_rs,
    cost_group_ss,
    cost_group_rs,
):
    rank, fields, rows, columns = sketch.shape
    halo = STEPS
    group = lax.axis_index("tm")
    band = lax.axis_index("lat")
    total_rows = rows * bands
    observed = station_row.shape[1] * bands
    tiles = columns // LANES

    loads = [
        pltpu.make_async_copy(source, target, load_sem.at[index])
        for index, (source, target) in enumerate(
            (
                (row_hbm, station_row),
                (column_hbm, station_column),
                (value_hbm, station_value),
                (stored_hbm, stored),
                (sketch_hbm.at[:, :1], sketch.at[:, :1]),
                (sketch_hbm.at[:, 1:], sketch.at[:, 1:]),
                (test_hbm, test),
            )
        )
    ]
    for load in loads[:6]:
        load.start()

    barrier = pltpu.get_barrier_semaphore()
    last_group = groups - 1

    def each(count, first, action):
        for index in range(first, count):
            action(index)

    def greet(place):
        pl.semaphore_signal(barrier, inc=1, device_id=place, device_id_type=MESH)

    @pl.when(group < last_group)
    def _():
        each(bands, 0, lambda index: greet({"tm": group + 1, "lat": index}))

    each(bands, 1, lambda offset: greet({"lat": lax.rem(band + offset, bands)}))

    for offset in range(2, groups):

        @pl.when(group + offset < groups)
        def _():
            greet({"tm": group + offset})

    for offset in range(1, groups):

        @pl.when(group - offset >= 0)
        def _():
            greet({"tm": group - offset})

    later = jnp.minimum(group, 1)
    greetings = bands - 1 + groups - 1 + (bands - 1) * later

    def remote(source, target, send_sem, recv_sem, where):
        return pltpu.make_async_remote_copy(
            src_ref=source,
            dst_ref=target,
            send_sem=send_sem,
            recv_sem=recv_sem,
            device_id=where,
            device_id_type=MESH,
        )

    below = {"lat": jnp.maximum(band - 1, 0)}
    above = {"lat": jnp.minimum(band + 1, bands - 1)}

    def halo_copies(send, recv, ss, rs, field):
        down = remote(send.at[0, field], recv.at[1, field], ss.at[0], rs.at[0], below)
        up = remote(send.at[1, field], recv.at[0, field], ss.at[0], rs.at[0], above)
        return down, up

    def halo_start(exchange, field):
        recv = exchange[1]
        down, up = halo_copies(*exchange, field)

        @pl.when(band > 0)
        def _():
            down.start()

        @pl.when(band == 0)
        def _():
            recv[0, field] = jnp.zeros(recv.shape[2:], recv.dtype)

        @pl.when(band < bands - 1)
        def _():
            up.start()

        @pl.when(band == bands - 1)
        def _():
            recv[1, field] = jnp.zeros(recv.shape[2:], recv.dtype)

    def both_or_one(action):
        @pl.when((band > 0) & (band < bands - 1))
        def _():
            action(slice(None))

        @pl.when(band == 0)
        def _():
            action(1)

        @pl.when(band == bands - 1)
        def _():
            action(0)

    def halo_wait(exchange):
        _, recv, ss, rs = exchange

        def one(place):
            remote(recv.at[place], recv.at[place], ss.at[0], rs.at[0], above).wait_recv()

        both_or_one(one)

    def halo_drain(exchange):
        send, _, ss, rs = exchange

        def one(place):
            remote(send.at[place], send.at[place], ss.at[0], rs.at[0], above).wait_send()

        both_or_one(one)

    base_halo = (base_send, base_recv, base_ss, base_rs)
    field_halo = (field_send, field_recv, field_ss, field_rs)
    last_halo = (last_send, last_recv, last_ss, last_rs)

    for load in loads[:4]:
        load.wait()

    base_half = stored[chosen[0]]
    base = base_half.astype(jnp.float32)
    base_send[0] = base[:, :halo]
    base_send[1] = base[:, rows - halo :]

    cells = lax.broadcasted_iota(jnp.int32, (columns, station_column.shape[1]), 0)
    at_column = cells == station_column[...]
    local_row = station_row[...] - band * rows
    at_row = (
        lax.broadcasted_iota(jnp.int32, (rows, station_row.shape[1]), 0) == local_row
    )
    one_hot = at_column.astype(jnp.float32).astype(jnp.bfloat16)
    by_row = jnp.dot(
        base_half[0],
        one_hot,
        preferred_element_type=jnp.float32,
    )
    seen = jnp.sum(jnp.where(at_row, by_row, 0.0), axis=0, keepdims=True)
    innovation = seen - station_value[...]
    weight = 1.0 + 2.0 * station_row[...].astype(jnp.float32) / total_rows
    weighted = weight * innovation
    cost = jnp.sum(weighted * innovation, axis=1, keepdims=True) / (2.0 * groups * observed)
    cost_row = jnp.broadcast_to(cost, (1, LANES))
    cost_out[...] = cost_row
    source = jnp.where(at_row, weighted / (2.0 * math.sqrt(observed)), 0.0)
    parts = [source.astype(jnp.bfloat16).astype(jnp.float32)]
    parts.append((source - parts[0]).astype(jnp.bfloat16).astype(jnp.float32))
    parts.append(source - parts[0] - parts[1])
    parts.append(jnp.zeros_like(source))
    placed = lax.dot_general(
        jnp.concatenate(parts, axis=0).astype(jnp.bfloat16),
        one_hot,
        (((1,), (1,)), ((), ())),
        preferred_element_type=jnp.float32,
    )
    forced[0] = placed[:rows] + placed[rows : 2 * rows] + placed[2 * rows : 3 * rows]
    for field in range(1, fields):
        forced[field] = jnp.zeros((rows, columns), jnp.float32)

    eye = lax.broadcasted_iota(jnp.int32, (rank, LANES), 0) == lax.broadcasted_iota(
        jnp.int32, (rank, LANES), 1
    )

    def spread_row(row):
        column = jnp.sum(jnp.where(eye, row, 0.0), axis=1, keepdims=True)
        spread[...] = jnp.broadcast_to(column, (rank, LANES))

    block = 8

    def combined(basis, field):
        def some(index, total):
            for inner in range(2 * block):
                k = index * 2 * block + inner
                factor = jnp.broadcast_to(spread[pl.ds(k, 1), :], (rows, LANES))
                total = total + basis[k, field].astype(jnp.float32) * jnp.concatenate(
                    [factor] * tiles, axis=1
                )
            return total

        return lax.fori_loop(
            0, rank // (2 * block), some, jnp.zeros((rows, columns), jnp.float32)
        )

    def fold(pairs, kept):
        def some(index, carry):
            totals = [None] * block
            for basis, values in pairs:
                for field in range(kept):
                    value = values[field]
                    for inner in range(block):
                        product = basis[index * block + inner, field].astype(jnp.float32) * value
                        for tile in range(tiles):
                            term = product[:, tile * LANES : (tile + 1) * LANES]
                            before = totals[inner]
                            totals[inner] = term if before is None else before + term
            for inner in range(block):
                folded[pl.ds(index * block + inner, 1), :] = jnp.sum(
                    totals[inner], axis=0, keepdims=True
                )
            return carry

        lax.fori_loop(0, rank // block, some, 0)
        share = jnp.sum(folded[...], axis=1, keepdims=True)
        message[...] = jnp.sum(jnp.where(eye, share, 0.0), axis=0, keepdims=True)

    def widen(source, target, start, stop):
        def some(index, carry):
            for inner in range(2):
                k = index * 2 + inner
                for field in range(fields):
                    target[k, field] = source[k, field].astype(jnp.float32)
            return carry

        lax.fori_loop(start // 2, stop // 2, some, 0)

    loads[4].wait()

    @pl.when(group < last_group)
    def _():
        loads[6].start()
        loads[5].wait()

    @pl.when(group == last_group)
    def _():
        fold(((sketch, forced),), 1)

    pl.semaphore_wait(barrier, greetings)

    def later_copy(offset):
        other = lax.rem(band + offset, bands)
        return remote(
            message,
            later_in.at[band],
            later_ss.at[0],
            later_rs.at[0],
            {"tm": jnp.maximum(group - 1, 0), "lat": other},
        )

    def own_copy(offset):
        other = lax.rem(band + offset, bands)
        return remote(
            message, own_in.at[band], own_ss.at[0], own_rs.at[0], {"lat": other}
        )

    def group_end(buffer, count, ss, rs):
        place = buffer.at[pl.ds(0, count)]
        return remote(place, place, ss.at[0], rs.at[0], {"lat": lax.rem(band + 1, bands)})

    def announce():
        @pl.when(group > 0)
        def _():
            each(bands, 0, lambda offset: later_copy(offset).start())

        each(bands, 1, lambda offset: own_copy(offset).start())
        own_in[band] = message[...]

    @pl.when(group == last_group)
    def _():
        announce()
        loads[5].wait()

    for field in range(fields):
        halo_start(base_halo, field)

    def cost_copy(offset):
        other = lax.rem(band + offset, bands)
        return remote(
            cost_out, cost_in.at[band], cost_ss.at[0], cost_rs.at[0], {"lat": other}
        )

    each(bands, 1, lambda offset: cost_copy(offset).start())
    cost_in[band] = cost_row

    def cost_group_copy(offset):
        other = lax.rem(group + offset, groups)
        return remote(
            cost_group_out,
            cost_group_in.at[group],
            cost_group_ss.at[0],
            cost_group_rs.at[0],
            {"tm": other},
        )

    def share_cost():
        group_end(cost_in, bands - 1, cost_ss, cost_rs).wait_recv()
        group_cost = jnp.sum(cost_in[...], axis=0)
        cost_group_out[...] = group_cost
        each(groups, 1, lambda offset: cost_group_copy(offset).start())
        cost_group_in[group] = group_cost

    low, high = pl.ds(0, halo), pl.ds(halo, halo)
    top = pl.ds(rows - halo, halo)
    early = rank * 3 // 4
    lots = (pl.ds(0, early), pl.ds(early, rank - early))

    def beyond_copies(lot):
        columns_of = lots[lot]
        return (
            remote(
                sketch.at[columns_of, :, low],
                beyond.at[columns_of, :, low],
                beyond_ss.at[lot],
                beyond_rs.at[lot],
                below,
            ),
            remote(
                sketch.at[columns_of, :, top],
                beyond.at[columns_of, :, high],
                beyond_ss.at[lot],
                beyond_rs.at[lot],
                above,
            ),
        )

    def beyond_end(lot):
        ends = {}

        def one(place):
            rows_of = pl.ds(0, 2 * halo) if isinstance(place, slice) else low
            part = beyond.at[lots[lot], :, rows_of]
            ends[0] = remote(part, part, beyond_ss.at[lot], beyond_rs.at[lot], above)

        return one, ends

    def beyond_wait(lot, sent):
        one, ends = beyond_end(lot)

        def wait(place):
            one(place)
            ends[0].wait_send() if sent else ends[0].wait_recv()

        both_or_one(wait)

    def clear(place):
        def one(k, carry):
            for field in range(fields):
                beyond[k, field, place] = jnp.zeros((halo, columns), beyond.dtype)
            return carry

        lax.fori_loop(0, rank, one, 0)

    @pl.when(group == 0)
    def _():
        @pl.when(band > 0)
        def _():
            for lot in range(2):
                beyond_copies(lot)[0].start()

        @pl.when(band == 0)
        def _():
            clear(high)

        @pl.when(band < bands - 1)
        def _():
            for lot in range(2):
                beyond_copies(lot)[1].start()

        @pl.when(band == bands - 1)
        def _():
            clear(low)

    @pl.when(group < last_group)
    def _():
        widen(sketch, sketch_wide, 0, rank)
        loads[6].wait()
        widen(test, test_wide, 0, rank)

    halo_wait(base_halo)
    scales = (0.5 * wave_coef * 0.25, 0.5 * flow_coef * 0.4, 0.5 * flow_coef * 0.4)
    starts = (0.5 * wave_coef, 0.0, 0.0)
    for field in range(fields):
        for place, part in (
            (pl.ds(0, rows), base[field]),
            (pl.ds(rows, halo), base_recv[1, field]),
            (pl.ds(rows + halo, halo), base_recv[0, field]),
        ):
            coef_ext[field, place] = starts[field] + scales[field] * part
    span = rows + 2 * halo
    inside = pl.ds(0, rows)
    after, before = pl.ds(rows, halo), pl.ds(rows + halo, halo)
    outside = pl.ds(rows, 2 * halo)

    def march(step_of, keep_outside):
        turned = lax.broadcasted_iota(jnp.int32, (span, LANES), 0)
        where = band * rows + jnp.where(turned < rows + halo, turned, turned - span)
        latitude = where.astype(jnp.float32)
        turn = wave_coef * coriolis_coef * (2.0 * (latitude + 0.5) / total_rows - 1.0)
        keep = jnp.where((where >= 0) & (where < total_rows), 1.0, 0.0)
        lane = lax.broadcasted_iota(jnp.int32, (span, LANES), 1)
        first, last = lane == 0, lane == LANES - 1

        def tiled(ref, field):
            return [ref[field, :, tile * LANES : (tile + 1) * LANES] for tile in range(tiles)]

        def dlon(values):
            ahead = [pltpu.roll(value, LANES - 1, 1) for value in values]
            behind = [pltpu.roll(value, 1, 1) for value in values]
            return [
                jnp.where(last, ahead[(tile + 1) % tiles], ahead[tile])
                - jnp.where(first, behind[tile - 1], behind[tile])
                for tile in range(tiles)
            ]

        coefs = [tiled(coef_ext, field) for field in range(fields)]
        source, target = ext, spare
        for step in range(STEPS):
            short = step == STEPS - 1 and not keep_outside
            state = [tiled(source, field) for field in range(fields)]
            for field, values in step_of(state, coefs, turn, dlon):
                for tile in range(tiles):
                    place = slice(tile * LANES, (tile + 1) * LANES)
                    value = values[tile] * keep
                    if short:
                        target[field, inside, place] = value[:rows]
                    else:
                        target[field, :, place] = value
            source, target = target, source

    def banded(basis, exchange):
        send, recv = exchange[:2]
        for field in range(fields):
            total = combined(basis, field)
            send[0, field] = total[:halo]
            send[1, field] = total[rows - halo :]
            halo_start(exchange, field)
            ext[field, inside] = total
        halo_wait(exchange)
        for field in range(fields):
            ext[field, before] = recv[0, field]
            ext[field, after] = recv[1, field]

    map_factor = map_scale / math.sqrt(rank * fields * total_rows * columns)

    def add_mapped():
        for field in range(fields):
            forced[field] = forced[field] + map_factor * ext[field, inside]

    @pl.when(group < last_group)
    def _():
        @pl.when(group < last_group - 1)
        def _():
            share_cost()

        @pl.when(group == 0)
        def _():
            beyond_wait(0, False)
            widen(beyond, beyond_wide, 0, early)
            beyond_wait(1, False)
            widen(beyond, beyond_wide, early, rank)

        group_end(later_in, bands, later_ss, later_rs).wait_recv()
        spread_row(jnp.sum(later_in[...], axis=0))

        @pl.when(group > 0)
        def _():
            banded(test_wide, field_halo)
            march(advance_adjoint, False)
            add_mapped()
            fold(((sketch_wide, forced),), fields)

        @pl.when(group == 0)
        def _():
            for field in range(fields):
                ext[field, inside] = combined(test_wide, field)
                ext[field, outside] = jnp.zeros((2 * halo, columns), jnp.float32)
            march(advance_adjoint, True)
            add_mapped()
            for field in range(fields):
                forced_beyond[field] = map_factor * ext[field, outside]

            fold(((sketch_wide, forced), (beyond_wide, forced_beyond)), fields)

        announce()

    @pl.when(group >= last_group - 1)
    def _():
        share_cost()

    group_end(cost_group_in, groups - 1, cost_group_ss, cost_group_rs).wait_recv()
    cost_here[...] = jnp.sum(cost_group_in[...], axis=0)[:, :1]
    group_end(own_in, bands - 1, own_ss, own_rs).wait_recv()
    adjoint_row = jnp.sum(own_in[...], axis=0)
    here = lax.broadcasted_iota(jnp.int32, (1, LANES), 1)
    adjoint[...] = jnp.where(here == rank, cost_here[...], adjoint_row)
    spread_row(adjoint_row)

    @pl.when(group > 0)
    def _():
        banded(sketch, last_halo)

    @pl.when(group == 0)
    def _():
        for field in range(fields):
            ext[field, inside] = combined(sketch_wide, field)
            ext[field, outside] = combined(beyond_wide, field)

    march(advance, False)
    for field in range(fields):
        increment[0, field] = ext[field, inside] / math.sqrt(rank)

    halo_drain(base_halo)
    group_end(cost_in, bands - 1, cost_ss, cost_rs).wait_send()
    group_end(own_in, bands - 1, own_ss, own_rs).wait_send()
    group_end(cost_group_in, groups - 1, cost_group_ss, cost_group_rs).wait_send()

    @pl.when(group > 0)
    def _():
        halo_drain(last_halo)
        group_end(later_in, bands, later_ss, later_rs).wait_send()

    @pl.when((group > 0) & (group < last_group))
    def _():
        halo_drain(field_halo)

    @pl.when(group == 0)
    def _():
        for lot in range(2):
            beyond_wait(lot, True)


def body(
    groups,
    bands,
    sketch,
    test_sketch,
    checkpoints,
    checkpoint_step,
    station_row,
    station_column,
    station_value,
):
    rank, fields, rows, columns = sketch.shape
    span = rows + 2 * STEPS
    f32 = jnp.float32

    def in_hbm(array):
        return pltpu.with_memory_space_constraint(array, pltpu.HBM)

    vmem = pl.BlockSpec(memory_space=pltpu.VMEM)
    hbm = pl.BlockSpec(memory_space=pltpu.HBM)
    edge = pltpu.VMEM((2, fields, STEPS, columns), f32)
    dma = pltpu.SemaphoreType.DMA
    increment, packed = pl.pallas_call(
        functools.partial(kernel, groups, bands),
        out_shape=(
            jax.ShapeDtypeStruct((1, fields, rows, columns), f32),
            jax.ShapeDtypeStruct((1, LANES), f32),
        ),
        in_specs=[hbm, hbm, hbm, pl.BlockSpec(memory_space=pltpu.SMEM), hbm, hbm, hbm],
        out_specs=(vmem, vmem),
        scratch_shapes=[
            pltpu.VMEM(sketch.shape, sketch.dtype),
            pltpu.VMEM(test_sketch.shape, test_sketch.dtype),
            pltpu.VMEM((rank, fields, 2 * STEPS, columns), sketch.dtype),
            pltpu.VMEM(sketch.shape, f32),
            pltpu.VMEM(test_sketch.shape, f32),
            pltpu.VMEM((rank, fields, 2 * STEPS, columns), f32),
            pltpu.VMEM(checkpoints.shape, checkpoints.dtype),
            pltpu.VMEM(station_row.shape, station_row.dtype),
            pltpu.VMEM(station_column.shape, station_column.dtype),
            pltpu.VMEM(station_value.shape, station_value.dtype),
            pltpu.VMEM((fields, span, columns), f32),
            pltpu.VMEM((fields, span, columns), f32),
            pltpu.VMEM((fields, span, columns), f32),
            pltpu.VMEM((fields, rows, columns), f32),
            pltpu.VMEM((fields, 2 * STEPS, columns), f32),
            pltpu.VMEM((rank, LANES), f32),
            pltpu.VMEM((rank, LANES), f32),
            edge,
            edge,
            edge,
            edge,
            edge,
            edge,
            pltpu.VMEM((1, LANES), f32),
            pltpu.VMEM((bands, 1, LANES), f32),
            pltpu.VMEM((bands, 1, LANES), f32),
            pltpu.VMEM((1, LANES), f32),
            pltpu.VMEM((bands, 1, LANES), f32),
            pltpu.VMEM((1, LANES), f32),
            pltpu.VMEM((groups, 1, LANES), f32),
            pltpu.VMEM((1, 1), f32),
            dma((8,)),
            dma((2,)),
            dma((2,)),
            dma((1,)),
            dma((1,)),
            dma((1,)),
            dma((1,)),
            dma((1,)),
            dma((1,)),
            dma((1,)),
            dma((1,)),
            dma((1,)),
            dma((1,)),
            dma((1,)),
            dma((1,)),
            dma((1,)),
            dma((1,)),
        ],
        compiler_params=pltpu.CompilerParams(
            collective_id=0,
            has_side_effects=True,
            vmem_limit_bytes=48 * 1024 * 1024,
        ),
    )(
        in_hbm(sketch),
        in_hbm(test_sketch),
        in_hbm(checkpoints),
        checkpoint_step,
        in_hbm(station_row),
        in_hbm(station_column),
        in_hbm(station_value),
    )
    keep = lax.broadcasted_iota(jnp.int32, packed.shape, 1) == rank
    return increment, packed[:, :rank], jnp.sum(jnp.where(keep, packed, 0.0))


def solution(mesh):
    placed = (
        P("tm", None, "lat", None),
        P("tm", None, "lat", None),
        P("tm", None, "lat", None),
        P("tm"),
        P("tm", "lat"),
        P("tm", "lat"),
        P("tm", "lat"),
    )
    return jax.shard_map(
        functools.partial(body, mesh.shape["tm"], mesh.shape["lat"]),
        mesh=mesh,
        in_specs=placed,
        out_specs=(P("tm", None, "lat", None), P("tm", None), P()),
        check_vma=False,
    )
```

```python
import functools
import math

import jax
import jax.numpy as jnp
from jax import lax
from jax.experimental import pallas as pl
from jax.experimental.pallas import tpu as pltpu
from jax.sharding import PartitionSpec as P

STEPS = 4
LANES = 128

wave_coef = 0.5
flow_coef = 0.4
coriolis_coef = 0.5
map_scale = 0.5

MESH = pl.DeviceIdType.MESH


def dlat(field):
    count = field.shape[0]
    return pltpu.roll(field, count - 1, 0) - pltpu.roll(field, 1, 0)


def advance(state, coefs, turn, dlon):
    half = 0.5 * wave_coef
    dx_height, dx_east, dx_north = (dlon(values) for values in state)
    out = [], [], []
    for tile, (height, east, north) in enumerate(zip(*state)):
        depth, east_flow, north_flow = (values[tile] for values in coefs)
        dy_north = dlat(north)
        dy_height = dlat(height)
        out[0].append(
            height
            - depth * (dx_east[tile] + dy_north)
            - (east_flow * dx_height[tile] + north_flow * dy_height)
        )
        out[1].append(
            east
            + turn * north
            - half * dx_height[tile]
            - (east_flow * dx_east[tile] + north_flow * dlat(east))
        )
        out[2].append(
            north
            - turn * east
            - half * dy_height
            - (east_flow * dx_north[tile] + north_flow * dy_north)
        )
    return enumerate(out)


def advance_adjoint(state, coefs, turn, dlon):
    half = 0.5 * wave_coef
    heights, easts, norths = state
    depths, east_flows, north_flows = coefs
    cells = list(zip(heights, easts, norths, depths, east_flows, north_flows))
    dx = dlon([half * u + e * h for h, u, v, d, e, n in cells])
    yield 0, [h + x + dlat(half * v + n * h) for x, (h, u, v, d, e, n) in zip(dx, cells)]
    dx = dlon([d * h + e * u for h, u, v, d, e, n in cells])
    yield 1, [u - turn * v + x + dlat(n * u) for x, (h, u, v, d, e, n) in zip(dx, cells)]
    dx = dlon([e * v for h, u, v, d, e, n in cells])
    yield 2, [v + turn * u + x + dlat(d * h + n * v) for x, (h, u, v, d, e, n) in zip(dx, cells)]


def kernel(
    groups,
    bands,
    sketch_hbm,
    test_hbm,
    stored_hbm,
    chosen,
    row_hbm,
    column_hbm,
    value_hbm,
    increment,
    adjoint,
    sketch,
    test,
    beyond,
    sketch_wide,
    test_wide,
    beyond_wide,
    beyond_rows,
    stored,
    station_row,
    station_column,
    station_value,
    coef_ext,
    ext,
    spare,
    forced,
    forced_beyond,
    folded,
    spread,
    base_send,
    base_recv,
    field_send,
    field_recv,
    last_send,
    last_recv,
    message,
    later_in,
    own_in,
    cost_out,
    cost_in,
    cost_group_out,
    cost_group_in,
    cost_here,
    load_sem,
    beyond_ss,
    beyond_rs,
    base_ss,
    base_rs,
    field_ss,
    field_rs,
    last_ss,
    last_rs,
    later_ss,
    later_rs,
    own_ss,
    own_rs,
    cost_ss,
    cost_rs,
    cost_group_ss,
    cost_group_rs,
):
    rank, fields, rows, columns = sketch.shape
    halo = STEPS
    group = lax.axis_index("tm")
    band = lax.axis_index("lat")
    total_rows = rows * bands
    observed = station_row.shape[1] * bands
    tiles = columns // LANES

    loads = [
        pltpu.make_async_copy(source, target, load_sem.at[index])
        for index, (source, target) in enumerate(
            (
                (row_hbm, station_row),
                (column_hbm, station_column),
                (value_hbm, station_value),
                (stored_hbm, stored),
                (sketch_hbm.at[:, :1], sketch.at[:, :1]),
                (sketch_hbm.at[:, 1:], sketch.at[:, 1:]),
                (test_hbm, test),
            )
        )
    ]
    for load in loads[:6]:
        load.start()

    barrier = pltpu.get_barrier_semaphore()
    last_group = groups - 1

    def each(count, first, action):
        for index in range(first, count):
            action(index)

    def greet(place):
        pl.semaphore_signal(barrier, inc=1, device_id=place, device_id_type=MESH)

    @pl.when(group < last_group)
    def _():
        each(bands, 0, lambda index: greet({"tm": group + 1, "lat": index}))

    each(bands, 1, lambda offset: greet({"lat": lax.rem(band + offset, bands)}))

    for offset in range(2, groups):

        @pl.when(group + offset < groups)
        def _():
            greet({"tm": group + offset})

    for offset in range(1, groups):

        @pl.when(group - offset >= 0)
        def _():
            greet({"tm": group - offset})

    later = jnp.minimum(group, 1)
    greetings = bands - 1 + groups - 1 + (bands - 1) * later

    def remote(source, target, send_sem, recv_sem, where):
        return pltpu.make_async_remote_copy(
            src_ref=source,
            dst_ref=target,
            send_sem=send_sem,
            recv_sem=recv_sem,
            device_id=where,
            device_id_type=MESH,
        )

    below = {"lat": jnp.maximum(band - 1, 0)}
    above = {"lat": jnp.minimum(band + 1, bands - 1)}

    def halo_copies(send, recv, ss, rs, field):
        down = remote(send.at[0, field], recv.at[1, field], ss.at[0], rs.at[0], below)
        up = remote(send.at[1, field], recv.at[0, field], ss.at[0], rs.at[0], above)
        return down, up

    def halo_start(exchange, field):
        recv = exchange[1]
        down, up = halo_copies(*exchange, field)

        @pl.when(band > 0)
        def _():
            down.start()

        @pl.when(band == 0)
        def _():
            recv[0, field] = jnp.zeros(recv.shape[2:], recv.dtype)

        @pl.when(band < bands - 1)
        def _():
            up.start()

        @pl.when(band == bands - 1)
        def _():
            recv[1, field] = jnp.zeros(recv.shape[2:], recv.dtype)

    def both_or_one(action):
        @pl.when((band > 0) & (band < bands - 1))
        def _():
            action(slice(None))

        @pl.when(band == 0)
        def _():
            action(1)

        @pl.when(band == bands - 1)
        def _():
            action(0)

    def halo_wait(exchange):
        _, recv, ss, rs = exchange

        def one(place):
            remote(recv.at[place], recv.at[place], ss.at[0], rs.at[0], above).wait_recv()

        both_or_one(one)

    def halo_drain(exchange):
        send, _, ss, rs = exchange

        def one(place):
            remote(send.at[place], send.at[place], ss.at[0], rs.at[0], above).wait_send()

        both_or_one(one)

    base_halo = (base_send, base_recv, base_ss, base_rs)
    field_halo = (field_send, field_recv, field_ss, field_rs)
    last_halo = (last_send, last_recv, last_ss, last_rs)

    for load in loads[:4]:
        load.wait()

    base_half = stored[chosen[0]]
    base = base_half.astype(jnp.float32)
    base_send[0] = base[:, :halo]
    base_send[1] = base[:, rows - halo :]

    cells = lax.broadcasted_iota(jnp.int32, (columns, station_column.shape[1]), 0)
    at_column = cells == station_column[...]
    local_row = station_row[...] - band * rows
    at_row = (
        lax.broadcasted_iota(jnp.int32, (rows, station_row.shape[1]), 0) == local_row
    )
    one_hot = at_column.astype(jnp.float32).astype(jnp.bfloat16)
    by_row = jnp.dot(
        base_half[0],
        one_hot,
        preferred_element_type=jnp.float32,
    )
    seen = jnp.sum(jnp.where(at_row, by_row, 0.0), axis=0, keepdims=True)
    innovation = seen - station_value[...]
    weight = 1.0 + 2.0 * station_row[...].astype(jnp.float32) / total_rows
    weighted = weight * innovation
    cost = jnp.sum(weighted * innovation, axis=1, keepdims=True) / (2.0 * groups * observed)
    cost_row = jnp.broadcast_to(cost, (1, LANES))
    cost_out[...] = cost_row
    source = jnp.where(at_row, weighted / (2.0 * math.sqrt(observed)), 0.0)
    parts = [source.astype(jnp.bfloat16).astype(jnp.float32)]
    parts.append((source - parts[0]).astype(jnp.bfloat16).astype(jnp.float32))
    parts.append(source - parts[0] - parts[1])
    parts.append(jnp.zeros_like(source))
    placed = lax.dot_general(
        jnp.concatenate(parts, axis=0).astype(jnp.bfloat16),
        one_hot,
        (((1,), (1,)), ((), ())),
        preferred_element_type=jnp.float32,
    )
    forced[0] = placed[:rows] + placed[rows : 2 * rows] + placed[2 * rows : 3 * rows]
    for field in range(1, fields):
        forced[field] = jnp.zeros((rows, columns), jnp.float32)

    eye = lax.broadcasted_iota(jnp.int32, (rank, LANES), 0) == lax.broadcasted_iota(
        jnp.int32, (rank, LANES), 1
    )

    per_tile = LANES // rows
    same_column = (
        lax.broadcasted_iota(jnp.int32, (per_tile, LANES), 1) // rows
        == lax.broadcasted_iota(jnp.int32, (per_tile, LANES), 0)
    )
    same_row = lax.broadcasted_iota(jnp.int32, (rows, LANES), 0) == lax.rem(
        lax.broadcasted_iota(jnp.int32, (rows, LANES), 1), rows
    )

    def spread_row(row, doubled):
        column = jnp.sum(jnp.where(eye, row, 0.0), axis=1, keepdims=True)
        spread[...] = jnp.broadcast_to(column, (rank, LANES))
        if not doubled:
            return None
        parts = []
        for tile in range(rank // per_tile):
            part = column[tile * per_tile : (tile + 1) * per_tile]
            line = jnp.sum(jnp.where(same_column, part, 0.0), axis=0, keepdims=True)
            square = jnp.where(same_row, line, 0.0)
            coarse = square.astype(jnp.bfloat16).astype(jnp.float32)
            parts.append(
                jnp.concatenate([coarse, square - coarse], axis=0).astype(jnp.bfloat16)
            )
        return jnp.concatenate(parts, axis=1)

    def by_matmul(left, basis_rows, field):
        both = jnp.dot(left, basis_rows[field], preferred_element_type=jnp.float32)
        return both[:rows] + both[rows:]

    def by_vector(basis, field):
        total = None
        for k in range(rank):
            factor = jnp.broadcast_to(spread[pl.ds(k, 1), :], (rows, LANES))
            term = basis[k, field].astype(jnp.float32) * jnp.concatenate([factor] * tiles, axis=1)
            total = term if total is None else total + term
        return total

    block = 8

    def combined(basis, field):
        def some(index, total):
            for inner in range(2 * block):
                k = index * 2 * block + inner
                factor = jnp.broadcast_to(spread[pl.ds(k, 1), :], (rows, LANES))
                total = total + basis[k, field].astype(jnp.float32) * jnp.concatenate(
                    [factor] * tiles, axis=1
                )
            return total

        return lax.fori_loop(
            0, rank // (2 * block), some, jnp.zeros((rows, columns), jnp.float32)
        )

    def fold_range(pairs, kept, start, stop):
        def some(index, carry):
            totals = [None] * block
            for basis, values in pairs:
                for field in range(kept):
                    value = values[field]
                    for inner in range(block):
                        product = basis[index * block + inner, field].astype(jnp.float32) * value
                        for tile in range(tiles):
                            term = product[:, tile * LANES : (tile + 1) * LANES]
                            before = totals[inner]
                            totals[inner] = term if before is None else before + term
            for inner in range(block):
                folded[pl.ds(index * block + inner, 1), :] = jnp.sum(
                    totals[inner], axis=0, keepdims=True
                )
            return carry

        lax.fori_loop(start // block, stop // block, some, 0)

    def fold_end():
        share = jnp.sum(folded[...], axis=1, keepdims=True)
        message[...] = jnp.sum(jnp.where(eye, share, 0.0), axis=0, keepdims=True)

    def widen(source, target, paired, start, stop):
        kept = 0 if paired is None else paired.shape[0]

        def some(index, carry):
            wides = []
            for inner in range(2):
                k = index * 2 + inner
                wide = [source[k, field].astype(jnp.float32) for field in range(fields)]
                if target is not None:
                    for field in range(fields):
                        target[k, field] = wide[field]
                wides.append(wide)
            place = pl.ds(pl.multiple_of(index * 2 * rows, 2 * rows), 2 * rows)
            for field in range(kept):
                paired[field, place] = jnp.concatenate(
                    [wide[field] for wide in wides], axis=0
                ).astype(jnp.bfloat16)
            return carry

        lax.fori_loop(start // 2, stop // 2, some, 0)

    loads[4].wait()

    @pl.when(group < last_group)
    def _():
        loads[6].start()
        loads[5].wait()

    @pl.when(group == last_group)
    def _():
        fold_range(((sketch, forced),), 1, 0, rank)
        fold_end()

    pl.semaphore_wait(barrier, greetings)

    def later_copy(offset):
        other = lax.rem(band + offset, bands)
        return remote(
            message,
            later_in.at[band],
            later_ss.at[0],
            later_rs.at[0],
            {"tm": jnp.maximum(group - 1, 0), "lat": other},
        )

    def own_copy(offset):
        other = lax.rem(band + offset, bands)
        return remote(
            message, own_in.at[band], own_ss.at[0], own_rs.at[0], {"lat": other}
        )

    def group_end(buffer, count, ss, rs):
        place = buffer.at[pl.ds(0, count)]
        return remote(place, place, ss.at[0], rs.at[0], {"lat": lax.rem(band + 1, bands)})

    def announce():
        @pl.when(group > 0)
        def _():
            each(bands, 0, lambda offset: later_copy(offset).start())

        each(bands, 1, lambda offset: own_copy(offset).start())
        own_in[band] = message[...]

    @pl.when(group == last_group)
    def _():
        announce()
        loads[5].wait()

    for field in range(fields):
        halo_start(base_halo, field)

    def cost_copy(offset):
        other = lax.rem(band + offset, bands)
        return remote(
            cost_out, cost_in.at[band], cost_ss.at[0], cost_rs.at[0], {"lat": other}
        )

    each(bands, 1, lambda offset: cost_copy(offset).start())
    cost_in[band] = cost_row

    def cost_group_copy(offset):
        other = lax.rem(group + offset, groups)
        return remote(
            cost_group_out,
            cost_group_in.at[group],
            cost_group_ss.at[0],
            cost_group_rs.at[0],
            {"tm": other},
        )

    def share_cost():
        group_end(cost_in, bands - 1, cost_ss, cost_rs).wait_recv()
        group_cost = jnp.sum(cost_in[...], axis=0)
        cost_group_out[...] = group_cost
        each(groups, 1, lambda offset: cost_group_copy(offset).start())
        cost_group_in[group] = group_cost

    low, high = pl.ds(0, halo), pl.ds(halo, halo)
    top = pl.ds(rows - halo, halo)
    early = rank * 3 // 4 // block * block
    lots = (pl.ds(0, early), pl.ds(early, rank - early))

    def beyond_copies(lot):
        columns_of = lots[lot]
        return (
            remote(
                sketch.at[columns_of, :, low],
                beyond.at[columns_of, :, low],
                beyond_ss.at[lot],
                beyond_rs.at[lot],
                below,
            ),
            remote(
                sketch.at[columns_of, :, top],
                beyond.at[columns_of, :, high],
                beyond_ss.at[lot],
                beyond_rs.at[lot],
                above,
            ),
        )

    def beyond_end(lot):
        ends = {}

        def one(place):
            rows_of = pl.ds(0, 2 * halo) if isinstance(place, slice) else low
            part = beyond.at[lots[lot], :, rows_of]
            ends[0] = remote(part, part, beyond_ss.at[lot], beyond_rs.at[lot], above)

        return one, ends

    def beyond_wait(lot, sent):
        one, ends = beyond_end(lot)

        def wait(place):
            one(place)
            ends[0].wait_send() if sent else ends[0].wait_recv()

        both_or_one(wait)

    def clear(place):
        def one(k, carry):
            for field in range(fields):
                beyond[k, field, place] = jnp.zeros((halo, columns), beyond.dtype)
            return carry

        lax.fori_loop(0, rank, one, 0)

    @pl.when(group == 0)
    def _():
        @pl.when(band > 0)
        def _():
            for lot in range(2):
                beyond_copies(lot)[0].start()

        @pl.when(band == 0)
        def _():
            clear(high)

        @pl.when(band < bands - 1)
        def _():
            for lot in range(2):
                beyond_copies(lot)[1].start()

        @pl.when(band == bands - 1)
        def _():
            clear(low)

    @pl.when(group < last_group)
    def _():
        widen(sketch, sketch_wide, None, 0, rank)
        loads[6].wait()
        widen(test, test_wide, None, 0, rank)

    halo_wait(base_halo)
    scales = (0.5 * wave_coef * 0.25, 0.5 * flow_coef * 0.4, 0.5 * flow_coef * 0.4)
    starts = (0.5 * wave_coef, 0.0, 0.0)
    for field in range(fields):
        for place, part in (
            (pl.ds(0, rows), base[field]),
            (pl.ds(rows, halo), base_recv[1, field]),
            (pl.ds(rows + halo, halo), base_recv[0, field]),
        ):
            coef_ext[field, place] = starts[field] + scales[field] * part
    span = rows + 2 * halo
    inside = pl.ds(0, rows)
    after, before = pl.ds(rows, halo), pl.ds(rows + halo, halo)
    outside = pl.ds(rows, 2 * halo)

    def march(step_of, keep_outside):
        turned = lax.broadcasted_iota(jnp.int32, (span, LANES), 0)
        where = band * rows + jnp.where(turned < rows + halo, turned, turned - span)
        latitude = where.astype(jnp.float32)
        turn = wave_coef * coriolis_coef * (2.0 * (latitude + 0.5) / total_rows - 1.0)
        keep = jnp.where((where >= 0) & (where < total_rows), 1.0, 0.0)
        lane = lax.broadcasted_iota(jnp.int32, (span, LANES), 1)
        first, last = lane == 0, lane == LANES - 1

        def tiled(ref, field):
            return [ref[field, :, tile * LANES : (tile + 1) * LANES] for tile in range(tiles)]

        def dlon(values):
            ahead = [pltpu.roll(value, LANES - 1, 1) for value in values]
            behind = [pltpu.roll(value, 1, 1) for value in values]
            return [
                jnp.where(last, ahead[(tile + 1) % tiles], ahead[tile])
                - jnp.where(first, behind[tile - 1], behind[tile])
                for tile in range(tiles)
            ]

        coefs = [tiled(coef_ext, field) for field in range(fields)]
        source, target = ext, spare
        for step in range(STEPS):
            short = step == STEPS - 1 and not keep_outside
            state = [tiled(source, field) for field in range(fields)]
            for field, values in step_of(state, coefs, turn, dlon):
                for tile in range(tiles):
                    place = slice(tile * LANES, (tile + 1) * LANES)
                    value = values[tile] * keep
                    if short:
                        target[field, inside, place] = value[:rows]
                    else:
                        target[field, :, place] = value
            source, target = target, source

    def banded(total_of, exchange):
        send, recv = exchange[:2]
        for field in range(fields):
            total = total_of(field)
            send[0, field] = total[:halo]
            send[1, field] = total[rows - halo :]
            halo_start(exchange, field)
            ext[field, inside] = total
        halo_wait(exchange)
        for field in range(fields):
            ext[field, before] = recv[0, field]
            ext[field, after] = recv[1, field]

    map_factor = map_scale / math.sqrt(rank * fields * total_rows * columns)

    def add_mapped():
        for field in range(fields):
            forced[field] = forced[field] + map_factor * ext[field, inside]

    @pl.when(group < last_group)
    def _():
        @pl.when(group < last_group - 1)
        def _():
            share_cost()

        @pl.when(group == 0)
        def _():
            beyond_wait(0, False)
            widen(beyond, beyond_wide, beyond_rows, 0, early)

        group_end(later_in, bands, later_ss, later_rs).wait_recv()
        spread_row(jnp.sum(later_in[...], axis=0), False)

        @pl.when(group > 0)
        def _():
            banded(lambda field: combined(test_wide, field), field_halo)
            march(advance_adjoint, False)
            add_mapped()
            fold_range(((sketch_wide, forced),), fields, 0, rank)
            fold_end()

        @pl.when(group == 0)
        def _():
            for field in range(fields):
                ext[field, inside] = combined(test_wide, field)
                ext[field, outside] = jnp.zeros((2 * halo, columns), jnp.float32)
            march(advance_adjoint, True)
            add_mapped()
            for field in range(fields):
                forced_beyond[field] = map_factor * ext[field, outside]

            fold_range(
                ((sketch_wide, forced), (beyond_wide, forced_beyond)), fields, 0, early
            )
            beyond_wait(1, False)
            fold_range(
                ((sketch_wide, forced), (beyond, forced_beyond)), fields, early, rank
            )
            fold_end()

        announce()

    @pl.when(group == 0)
    def _():
        widen(beyond, None, beyond_rows, early, rank)

    @pl.when(group >= last_group - 1)
    def _():
        share_cost()

    group_end(cost_group_in, groups - 1, cost_group_ss, cost_group_rs).wait_recv()
    cost_here[...] = jnp.sum(cost_group_in[...], axis=0)[:, :1]
    group_end(own_in, bands - 1, own_ss, own_rs).wait_recv()
    adjoint_row = jnp.sum(own_in[...], axis=0)
    left_own = spread_row(adjoint_row, True)
    here = lax.broadcasted_iota(jnp.int32, (1, LANES), 1)
    adjoint[...] = jnp.where(here == rank, cost_here[...], adjoint_row)

    @pl.when(group > 0)
    def _():
        banded(lambda field: combined(sketch, field), last_halo)

    @pl.when(group == 0)
    def _():
        for field in range(fields):
            ext[field, outside] = by_matmul(left_own, beyond_rows, field)
            own = sketch if field == fields - 1 else sketch_wide
            ext[field, inside] = by_vector(own, field)

    march(advance, False)
    for field in range(fields):
        increment[0, field] = ext[field, inside] / math.sqrt(rank)

    halo_drain(base_halo)
    group_end(cost_in, bands - 1, cost_ss, cost_rs).wait_send()
    group_end(own_in, bands - 1, own_ss, own_rs).wait_send()
    group_end(cost_group_in, groups - 1, cost_group_ss, cost_group_rs).wait_send()

    @pl.when(group > 0)
    def _():
        halo_drain(last_halo)
        group_end(later_in, bands, later_ss, later_rs).wait_send()

    @pl.when((group > 0) & (group < last_group))
    def _():
        halo_drain(field_halo)

    @pl.when(group == 0)
    def _():
        for lot in range(2):
            beyond_wait(lot, True)


def body(
    groups,
    bands,
    sketch,
    test_sketch,
    checkpoints,
    checkpoint_step,
    station_row,
    station_column,
    station_value,
):
    rank, fields, rows, columns = sketch.shape
    span = rows + 2 * STEPS
    f32 = jnp.float32

    def in_hbm(array):
        return pltpu.with_memory_space_constraint(array, pltpu.HBM)

    vmem = pl.BlockSpec(memory_space=pltpu.VMEM)
    hbm = pl.BlockSpec(memory_space=pltpu.HBM)
    edge = pltpu.VMEM((2, fields, STEPS, columns), f32)
    dma = pltpu.SemaphoreType.DMA
    increment, packed = pl.pallas_call(
        functools.partial(kernel, groups, bands),
        out_shape=(
            jax.ShapeDtypeStruct((1, fields, rows, columns), f32),
            jax.ShapeDtypeStruct((1, LANES), f32),
        ),
        in_specs=[hbm, hbm, hbm, pl.BlockSpec(memory_space=pltpu.SMEM), hbm, hbm, hbm],
        out_specs=(vmem, vmem),
        scratch_shapes=[
            pltpu.VMEM(sketch.shape, sketch.dtype),
            pltpu.VMEM(test_sketch.shape, test_sketch.dtype),
            pltpu.VMEM((rank, fields, 2 * STEPS, columns), sketch.dtype),
            pltpu.VMEM(sketch.shape, f32),
            pltpu.VMEM(test_sketch.shape, f32),
            pltpu.VMEM((rank, fields, 2 * STEPS, columns), f32),
            pltpu.VMEM((fields, rank * 2 * STEPS, columns), sketch.dtype),
            pltpu.VMEM(checkpoints.shape, checkpoints.dtype),
            pltpu.VMEM(station_row.shape, station_row.dtype),
            pltpu.VMEM(station_column.shape, station_column.dtype),
            pltpu.VMEM(station_value.shape, station_value.dtype),
            pltpu.VMEM((fields, span, columns), f32),
            pltpu.VMEM((fields, span, columns), f32),
            pltpu.VMEM((fields, span, columns), f32),
            pltpu.VMEM((fields, rows, columns), f32),
            pltpu.VMEM((fields, 2 * STEPS, columns), f32),
            pltpu.VMEM((rank, LANES), f32),
            pltpu.VMEM((rank, LANES), f32),
            edge,
            edge,
            edge,
            edge,
            edge,
            edge,
            pltpu.VMEM((1, LANES), f32),
            pltpu.VMEM((bands, 1, LANES), f32),
            pltpu.VMEM((bands, 1, LANES), f32),
            pltpu.VMEM((1, LANES), f32),
            pltpu.VMEM((bands, 1, LANES), f32),
            pltpu.VMEM((1, LANES), f32),
            pltpu.VMEM((groups, 1, LANES), f32),
            pltpu.VMEM((1, 1), f32),
            dma((8,)),
            dma((2,)),
            dma((2,)),
            dma((1,)),
            dma((1,)),
            dma((1,)),
            dma((1,)),
            dma((1,)),
            dma((1,)),
            dma((1,)),
            dma((1,)),
            dma((1,)),
            dma((1,)),
            dma((1,)),
            dma((1,)),
            dma((1,)),
            dma((1,)),
        ],
        compiler_params=pltpu.CompilerParams(
            collective_id=0,
            has_side_effects=True,
            vmem_limit_bytes=48 * 1024 * 1024,
        ),
    )(
        in_hbm(sketch),
        in_hbm(test_sketch),
        in_hbm(checkpoints),
        checkpoint_step,
        in_hbm(station_row),
        in_hbm(station_column),
        in_hbm(station_value),
    )
    keep = lax.broadcasted_iota(jnp.int32, packed.shape, 1) == rank
    return increment, packed[:, :rank], jnp.sum(jnp.where(keep, packed, 0.0))


def solution(mesh):
    placed = (
        P("tm", None, "lat", None),
        P("tm", None, "lat", None),
        P("tm", None, "lat", None),
        P("tm"),
        P("tm", "lat"),
        P("tm", "lat"),
        P("tm", "lat"),
    )
    return jax.shard_map(
        functools.partial(body, mesh.shape["tm"], mesh.shape["lat"]),
        mesh=mesh,
        in_specs=placed,
        out_specs=(P("tm", None, "lat", None), P("tm", None), P()),
        check_vma=False,
    )
```

```python
import functools
import math

import jax
import jax.numpy as jnp
from jax import lax
from jax.experimental import pallas as pl
from jax.experimental.pallas import tpu as pltpu
from jax.sharding import PartitionSpec as P

STEPS = 4
LANES = 128

wave_coef = 0.5
flow_coef = 0.4
coriolis_coef = 0.5
map_scale = 0.5

MESH = pl.DeviceIdType.MESH


def dlat(field):
    count = field.shape[0]
    return pltpu.roll(field, count - 1, 0) - pltpu.roll(field, 1, 0)


def advance(state, coefs, turn, dlon):
    half = 0.5 * wave_coef
    dx_height, dx_east, dx_north = (dlon(values) for values in state)
    out = [], [], []
    for tile, (height, east, north) in enumerate(zip(*state)):
        depth, east_flow, north_flow = (values[tile] for values in coefs)
        dy_north = dlat(north)
        dy_height = dlat(height)
        out[0].append(
            height
            - depth * (dx_east[tile] + dy_north)
            - (east_flow * dx_height[tile] + north_flow * dy_height)
        )
        out[1].append(
            east
            + turn * north
            - half * dx_height[tile]
            - (east_flow * dx_east[tile] + north_flow * dlat(east))
        )
        out[2].append(
            north
            - turn * east
            - half * dy_height
            - (east_flow * dx_north[tile] + north_flow * dy_north)
        )
    return enumerate(out)


def advance_adjoint(state, coefs, turn, dlon):
    half = 0.5 * wave_coef
    heights, easts, norths = state
    depths, east_flows, north_flows = coefs
    cells = list(zip(heights, easts, norths, depths, east_flows, north_flows))
    dx = dlon([half * u + e * h for h, u, v, d, e, n in cells])
    yield 0, [h + x + dlat(half * v + n * h) for x, (h, u, v, d, e, n) in zip(dx, cells)]
    dx = dlon([d * h + e * u for h, u, v, d, e, n in cells])
    yield 1, [u - turn * v + x + dlat(n * u) for x, (h, u, v, d, e, n) in zip(dx, cells)]
    dx = dlon([e * v for h, u, v, d, e, n in cells])
    yield 2, [v + turn * u + x + dlat(d * h + n * v) for x, (h, u, v, d, e, n) in zip(dx, cells)]


def kernel(
    groups,
    bands,
    sketch_hbm,
    test_hbm,
    stored_hbm,
    chosen,
    row_hbm,
    column_hbm,
    value_hbm,
    increment,
    adjoint,
    sketch,
    test,
    beyond,
    sketch_wide,
    test_wide,
    beyond_wide,
    beyond_rows,
    stored,
    station_row,
    station_column,
    station_value,
    coef_ext,
    ext,
    spare,
    forced,
    forced_beyond,
    folded,
    spread,
    base_send,
    base_recv,
    field_send,
    field_recv,
    last_send,
    last_recv,
    message,
    later_in,
    own_in,
    cost_out,
    cost_in,
    cost_group_out,
    cost_group_in,
    cost_here,
    load_sem,
    beyond_ss,
    beyond_rs,
    base_ss,
    base_rs,
    field_ss,
    field_rs,
    last_ss,
    last_rs,
    later_ss,
    later_rs,
    own_ss,
    own_rs,
    cost_ss,
    cost_rs,
    cost_group_ss,
    cost_group_rs,
):
    rank, fields, rows, columns = sketch.shape
    halo = STEPS
    group = lax.axis_index("tm")
    band = lax.axis_index("lat")
    total_rows = rows * bands
    observed = station_row.shape[1] * bands
    tiles = columns // LANES

    loads = [
        pltpu.make_async_copy(source, target, load_sem.at[index])
        for index, (source, target) in enumerate(
            (
                (row_hbm, station_row),
                (column_hbm, station_column),
                (value_hbm, station_value),
                (stored_hbm, stored),
                (sketch_hbm.at[:, :1], sketch.at[:, :1]),
                (sketch_hbm.at[:, 1:], sketch.at[:, 1:]),
                (test_hbm, test),
            )
        )
    ]
    barrier = pltpu.get_barrier_semaphore()
    last_group = groups - 1

    def each(count, first, action):
        for index in range(first, count):
            action(index)

    def greet(place):
        pl.semaphore_signal(barrier, inc=1, device_id=place, device_id_type=MESH)

    @pl.when(group < last_group)
    def _():
        each(bands, 0, lambda index: greet({"tm": group + 1, "lat": index}))

    each(bands, 1, lambda offset: greet({"lat": lax.rem(band + offset, bands)}))

    for offset in range(2, groups):

        @pl.when(group + offset < groups)
        def _():
            greet({"tm": group + offset})

    for offset in range(1, groups):

        @pl.when(group - offset >= 0)
        def _():
            greet({"tm": group - offset})

    for load in loads[:6]:
        load.start()

    later = jnp.minimum(group, 1)
    greetings = bands - 1 + groups - 1 + (bands - 1) * later

    def remote(source, target, send_sem, recv_sem, where):
        return pltpu.make_async_remote_copy(
            src_ref=source,
            dst_ref=target,
            send_sem=send_sem,
            recv_sem=recv_sem,
            device_id=where,
            device_id_type=MESH,
        )

    below = {"lat": jnp.maximum(band - 1, 0)}
    above = {"lat": jnp.minimum(band + 1, bands - 1)}

    def halo_copies(send, recv, ss, rs, field):
        down = remote(send.at[0, field], recv.at[1, field], ss.at[0], rs.at[0], below)
        up = remote(send.at[1, field], recv.at[0, field], ss.at[0], rs.at[0], above)
        return down, up

    def halo_start(exchange, field):
        recv = exchange[1]
        down, up = halo_copies(*exchange, field)

        @pl.when(band > 0)
        def _():
            down.start()

        @pl.when(band == 0)
        def _():
            recv[0, field] = jnp.zeros(recv.shape[2:], recv.dtype)

        @pl.when(band < bands - 1)
        def _():
            up.start()

        @pl.when(band == bands - 1)
        def _():
            recv[1, field] = jnp.zeros(recv.shape[2:], recv.dtype)

    def both_or_one(action):
        @pl.when((band > 0) & (band < bands - 1))
        def _():
            action(slice(None))

        @pl.when(band == 0)
        def _():
            action(1)

        @pl.when(band == bands - 1)
        def _():
            action(0)

    def halo_wait(exchange):
        _, recv, ss, rs = exchange

        def one(place):
            remote(recv.at[place], recv.at[place], ss.at[0], rs.at[0], above).wait_recv()

        both_or_one(one)

    def halo_drain(exchange):
        send, _, ss, rs = exchange

        def one(place):
            remote(send.at[place], send.at[place], ss.at[0], rs.at[0], above).wait_send()

        both_or_one(one)

    base_halo = (base_send, base_recv, base_ss, base_rs)
    field_halo = (field_send, field_recv, field_ss, field_rs)
    last_halo = (last_send, last_recv, last_ss, last_rs)

    for load in loads[:4]:
        load.wait()

    base_half = stored[chosen[0]]
    base = base_half.astype(jnp.float32)
    base_send[0] = base[:, :halo]
    base_send[1] = base[:, rows - halo :]

    cells = lax.broadcasted_iota(jnp.int32, (columns, station_column.shape[1]), 0)
    at_column = cells == station_column[...]
    local_row = station_row[...] - band * rows
    at_row = (
        lax.broadcasted_iota(jnp.int32, (rows, station_row.shape[1]), 0) == local_row
    )
    one_hot = at_column.astype(jnp.float32).astype(jnp.bfloat16)
    by_row = jnp.dot(
        base_half[0],
        one_hot,
        preferred_element_type=jnp.float32,
    )
    seen = jnp.sum(jnp.where(at_row, by_row, 0.0), axis=0, keepdims=True)
    innovation = seen - station_value[...]
    weight = 1.0 + 2.0 * station_row[...].astype(jnp.float32) / total_rows
    weighted = weight * innovation
    cost = jnp.sum(weighted * innovation, axis=1, keepdims=True) / (2.0 * groups * observed)
    cost_row = jnp.broadcast_to(cost, (1, LANES))
    cost_out[...] = cost_row
    source = jnp.where(at_row, weighted / (2.0 * math.sqrt(observed)), 0.0)
    parts = [source.astype(jnp.bfloat16).astype(jnp.float32)]
    parts.append((source - parts[0]).astype(jnp.bfloat16).astype(jnp.float32))
    parts.append(source - parts[0] - parts[1])
    parts.append(jnp.zeros_like(source))
    placed = lax.dot_general(
        jnp.concatenate(parts, axis=0).astype(jnp.bfloat16),
        one_hot,
        (((1,), (1,)), ((), ())),
        preferred_element_type=jnp.float32,
    )
    forced[0] = placed[:rows] + placed[rows : 2 * rows] + placed[2 * rows : 3 * rows]
    for field in range(1, fields):
        forced[field] = jnp.zeros((rows, columns), jnp.float32)

    eye = lax.broadcasted_iota(jnp.int32, (rank, LANES), 0) == lax.broadcasted_iota(
        jnp.int32, (rank, LANES), 1
    )

    per_tile = LANES // rows
    same_column = (
        lax.broadcasted_iota(jnp.int32, (per_tile, LANES), 1) // rows
        == lax.broadcasted_iota(jnp.int32, (per_tile, LANES), 0)
    )
    same_row = lax.broadcasted_iota(jnp.int32, (rows, LANES), 0) == lax.rem(
        lax.broadcasted_iota(jnp.int32, (rows, LANES), 1), rows
    )

    def spread_row(row, doubled):
        column = jnp.sum(jnp.where(eye, row, 0.0), axis=1, keepdims=True)
        spread[...] = jnp.broadcast_to(column, (rank, LANES))
        if not doubled:
            return None
        parts = []
        for tile in range(rank // per_tile):
            part = column[tile * per_tile : (tile + 1) * per_tile]
            line = jnp.sum(jnp.where(same_column, part, 0.0), axis=0, keepdims=True)
            square = jnp.where(same_row, line, 0.0)
            coarse = square.astype(jnp.bfloat16).astype(jnp.float32)
            parts.append(
                jnp.concatenate([coarse, square - coarse], axis=0).astype(jnp.bfloat16)
            )
        return jnp.concatenate(parts, axis=1)

    def by_matmul(left, basis_rows, field):
        both = jnp.dot(left, basis_rows[field], preferred_element_type=jnp.float32)
        return both[:rows] + both[rows:]

    def by_vector(basis, field):
        total = None
        for k in range(rank):
            factor = jnp.broadcast_to(spread[pl.ds(k, 1), :], (rows, LANES))
            term = basis[k, field].astype(jnp.float32) * jnp.concatenate([factor] * tiles, axis=1)
            total = term if total is None else total + term
        return total

    block = 8

    def combined(basis, field):
        def some(index, total):
            for inner in range(2 * block):
                k = index * 2 * block + inner
                factor = jnp.broadcast_to(spread[pl.ds(k, 1), :], (rows, LANES))
                total = total + basis[k, field].astype(jnp.float32) * jnp.concatenate(
                    [factor] * tiles, axis=1
                )
            return total

        return lax.fori_loop(
            0, rank // (2 * block), some, jnp.zeros((rows, columns), jnp.float32)
        )

    def fold_range(pairs, kept, start, stop):
        def some(index, carry):
            totals = [None] * block
            for basis, values in pairs:
                for field in range(kept):
                    value = values[field]
                    for inner in range(block):
                        product = basis[index * block + inner, field].astype(jnp.float32) * value
                        for tile in range(tiles):
                            term = product[:, tile * LANES : (tile + 1) * LANES]
                            before = totals[inner]
                            totals[inner] = term if before is None else before + term
            for inner in range(block):
                folded[pl.ds(index * block + inner, 1), :] = jnp.sum(
                    totals[inner], axis=0, keepdims=True
                )
            return carry

        lax.fori_loop(start // block, stop // block, some, 0)

    def fold_end():
        share = jnp.sum(folded[...], axis=1, keepdims=True)
        message[...] = jnp.sum(jnp.where(eye, share, 0.0), axis=0, keepdims=True)

    def widen(source, target, paired, start, stop):
        kept = 0 if paired is None else paired.shape[0]

        def some(index, carry):
            wides = []
            for inner in range(2):
                k = index * 2 + inner
                wide = [source[k, field].astype(jnp.float32) for field in range(fields)]
                if target is not None:
                    for field in range(fields):
                        target[k, field] = wide[field]
                wides.append(wide)
            place = pl.ds(pl.multiple_of(index * 2 * rows, 2 * rows), 2 * rows)
            for field in range(kept):
                paired[field, place] = jnp.concatenate(
                    [wide[field] for wide in wides], axis=0
                ).astype(jnp.bfloat16)
            return carry

        lax.fori_loop(start // 2, stop // 2, some, 0)

    loads[4].wait()

    @pl.when(group < last_group)
    def _():
        loads[6].start()
        loads[5].wait()

    @pl.when(group == last_group)
    def _():
        fold_range(((sketch, forced),), 1, 0, rank)
        fold_end()

    pl.semaphore_wait(barrier, greetings)

    def later_copy(offset):
        other = lax.rem(band + offset, bands)
        return remote(
            message,
            later_in.at[band],
            later_ss.at[0],
            later_rs.at[0],
            {"tm": jnp.maximum(group - 1, 0), "lat": other},
        )

    def own_copy(offset):
        other = lax.rem(band + offset, bands)
        return remote(
            message, own_in.at[band], own_ss.at[0], own_rs.at[0], {"lat": other}
        )

    def group_end(buffer, count, ss, rs):
        place = buffer.at[pl.ds(0, count)]
        return remote(place, place, ss.at[0], rs.at[0], {"lat": lax.rem(band + 1, bands)})

    def announce():
        @pl.when(group > 0)
        def _():
            each(bands, 0, lambda offset: later_copy(offset).start())

        each(bands, 1, lambda offset: own_copy(offset).start())
        own_in[band] = message[...]

    @pl.when(group == last_group)
    def _():
        announce()
        loads[5].wait()

    for field in range(fields):
        halo_start(base_halo, field)

    def cost_copy(offset):
        other = lax.rem(band + offset, bands)
        return remote(
            cost_out, cost_in.at[band], cost_ss.at[0], cost_rs.at[0], {"lat": other}
        )

    each(bands, 1, lambda offset: cost_copy(offset).start())
    cost_in[band] = cost_row

    def cost_group_copy(offset):
        other = lax.rem(group + offset, groups)
        return remote(
            cost_group_out,
            cost_group_in.at[group],
            cost_group_ss.at[0],
            cost_group_rs.at[0],
            {"tm": other},
        )

    def share_cost():
        group_end(cost_in, bands - 1, cost_ss, cost_rs).wait_recv()
        group_cost = jnp.sum(cost_in[...], axis=0)
        cost_group_out[...] = group_cost
        each(groups, 1, lambda offset: cost_group_copy(offset).start())
        cost_group_in[group] = group_cost

    low, high = pl.ds(0, halo), pl.ds(halo, halo)
    top = pl.ds(rows - halo, halo)
    early = rank * 3 // 4 // block * block
    lots = (pl.ds(0, early), pl.ds(early, rank - early))

    def beyond_copies(lot):
        columns_of = lots[lot]
        return (
            remote(
                sketch.at[columns_of, :, low],
                beyond.at[columns_of, :, low],
                beyond_ss.at[lot],
                beyond_rs.at[lot],
                below,
            ),
            remote(
                sketch.at[columns_of, :, top],
                beyond.at[columns_of, :, high],
                beyond_ss.at[lot],
                beyond_rs.at[lot],
                above,
            ),
        )

    def beyond_end(lot):
        ends = {}

        def one(place):
            rows_of = pl.ds(0, 2 * halo) if isinstance(place, slice) else low
            part = beyond.at[lots[lot], :, rows_of]
            ends[0] = remote(part, part, beyond_ss.at[lot], beyond_rs.at[lot], above)

        return one, ends

    def beyond_wait(lot, sent):
        one, ends = beyond_end(lot)

        def wait(place):
            one(place)
            ends[0].wait_send() if sent else ends[0].wait_recv()

        both_or_one(wait)

    def clear(place):
        def one(k, carry):
            for field in range(fields):
                beyond[k, field, place] = jnp.zeros((halo, columns), beyond.dtype)
            return carry

        lax.fori_loop(0, rank, one, 0)

    @pl.when(group == 0)
    def _():
        @pl.when(band > 0)
        def _():
            for lot in range(2):
                beyond_copies(lot)[0].start()

        @pl.when(band == 0)
        def _():
            clear(high)

        @pl.when(band < bands - 1)
        def _():
            for lot in range(2):
                beyond_copies(lot)[1].start()

        @pl.when(band == bands - 1)
        def _():
            clear(low)

    @pl.when(group < last_group)
    def _():
        widen(sketch, sketch_wide, None, 0, rank)
        loads[6].wait()
        widen(test, test_wide, None, 0, rank)

    halo_wait(base_halo)
    scales = (0.5 * wave_coef * 0.25, 0.5 * flow_coef * 0.4, 0.5 * flow_coef * 0.4)
    starts = (0.5 * wave_coef, 0.0, 0.0)
    for field in range(fields):
        for place, part in (
            (pl.ds(0, rows), base[field]),
            (pl.ds(rows, halo), base_recv[1, field]),
            (pl.ds(rows + halo, halo), base_recv[0, field]),
        ):
            coef_ext[field, place] = starts[field] + scales[field] * part
    span = rows + 2 * halo
    inside = pl.ds(0, rows)
    after, before = pl.ds(rows, halo), pl.ds(rows + halo, halo)
    outside = pl.ds(rows, 2 * halo)

    def march(step_of, keep_outside):
        turned = lax.broadcasted_iota(jnp.int32, (span, LANES), 0)
        where = band * rows + jnp.where(turned < rows + halo, turned, turned - span)
        latitude = where.astype(jnp.float32)
        turn = wave_coef * coriolis_coef * (2.0 * (latitude + 0.5) / total_rows - 1.0)
        keep = jnp.where((where >= 0) & (where < total_rows), 1.0, 0.0)
        lane = lax.broadcasted_iota(jnp.int32, (span, LANES), 1)
        first, last = lane == 0, lane == LANES - 1

        def tiled(ref, field):
            return [ref[field, :, tile * LANES : (tile + 1) * LANES] for tile in range(tiles)]

        def dlon(values):
            ahead = [pltpu.roll(value, LANES - 1, 1) for value in values]
            behind = [pltpu.roll(value, 1, 1) for value in values]
            return [
                jnp.where(last, ahead[(tile + 1) % tiles], ahead[tile])
                - jnp.where(first, behind[tile - 1], behind[tile])
                for tile in range(tiles)
            ]

        coefs = [tiled(coef_ext, field) for field in range(fields)]
        source, target = ext, spare
        for step in range(STEPS):
            short = step == STEPS - 1 and not keep_outside
            state = [tiled(source, field) for field in range(fields)]
            for field, values in step_of(state, coefs, turn, dlon):
                for tile in range(tiles):
                    place = slice(tile * LANES, (tile + 1) * LANES)
                    value = values[tile] * keep
                    if short:
                        target[field, inside, place] = value[:rows]
                    else:
                        target[field, :, place] = value
            source, target = target, source

    def banded(total_of, exchange):
        send, recv = exchange[:2]
        for field in range(fields):
            total = total_of(field)
            send[0, field] = total[:halo]
            send[1, field] = total[rows - halo :]
            halo_start(exchange, field)
            ext[field, inside] = total
        halo_wait(exchange)
        for field in range(fields):
            ext[field, before] = recv[0, field]
            ext[field, after] = recv[1, field]

    map_factor = map_scale / math.sqrt(rank * fields * total_rows * columns)

    def add_mapped():
        for field in range(fields):
            forced[field] = forced[field] + map_factor * ext[field, inside]

    @pl.when(group < last_group)
    def _():
        @pl.when(group < last_group - 1)
        def _():
            share_cost()

        @pl.when(group == 0)
        def _():
            beyond_wait(0, False)
            widen(beyond, beyond_wide, beyond_rows, 0, early)

        group_end(later_in, bands, later_ss, later_rs).wait_recv()
        spread_row(jnp.sum(later_in[...], axis=0), False)

        @pl.when(group > 0)
        def _():
            banded(lambda field: combined(test_wide, field), field_halo)
            march(advance_adjoint, False)
            add_mapped()
            fold_range(((sketch_wide, forced),), fields, 0, rank)
            fold_end()

        @pl.when(group == 0)
        def _():
            for field in range(fields):
                ext[field, inside] = combined(test_wide, field)
                ext[field, outside] = jnp.zeros((2 * halo, columns), jnp.float32)
            march(advance_adjoint, True)
            add_mapped()
            for field in range(fields):
                forced_beyond[field] = map_factor * ext[field, outside]

            fold_range(
                ((sketch_wide, forced), (beyond_wide, forced_beyond)), fields, 0, early
            )
            beyond_wait(1, False)
            fold_range(
                ((sketch_wide, forced), (beyond, forced_beyond)), fields, early, rank
            )
            fold_end()

        announce()

    @pl.when(group == 0)
    def _():
        widen(beyond, None, beyond_rows, early, rank)

    @pl.when(group >= last_group - 1)
    def _():
        share_cost()

    group_end(cost_group_in, groups - 1, cost_group_ss, cost_group_rs).wait_recv()
    cost_here[...] = jnp.sum(cost_group_in[...], axis=0)[:, :1]
    group_end(own_in, bands - 1, own_ss, own_rs).wait_recv()
    adjoint_row = jnp.sum(own_in[...], axis=0)
    left_own = spread_row(adjoint_row, True)
    here = lax.broadcasted_iota(jnp.int32, (1, LANES), 1)
    adjoint[...] = jnp.where(here == rank, cost_here[...], adjoint_row)

    @pl.when(group > 0)
    def _():
        banded(lambda field: combined(sketch, field), last_halo)

    @pl.when(group == 0)
    def _():
        for field in range(fields):
            ext[field, outside] = by_matmul(left_own, beyond_rows, field)
            own = sketch if field == fields - 1 else sketch_wide
            ext[field, inside] = by_vector(own, field)

    march(advance, False)
    for field in range(fields):
        increment[0, field] = ext[field, inside] / math.sqrt(rank)

    halo_drain(base_halo)
    group_end(cost_in, bands - 1, cost_ss, cost_rs).wait_send()
    group_end(own_in, bands - 1, own_ss, own_rs).wait_send()
    group_end(cost_group_in, groups - 1, cost_group_ss, cost_group_rs).wait_send()

    @pl.when(group > 0)
    def _():
        halo_drain(last_halo)
        group_end(later_in, bands, later_ss, later_rs).wait_send()

    @pl.when((group > 0) & (group < last_group))
    def _():
        halo_drain(field_halo)

    @pl.when(group == 0)
    def _():
        for lot in range(2):
            beyond_wait(lot, True)


def body(
    groups,
    bands,
    sketch,
    test_sketch,
    checkpoints,
    checkpoint_step,
    station_row,
    station_column,
    station_value,
):
    rank, fields, rows, columns = sketch.shape
    span = rows + 2 * STEPS
    f32 = jnp.float32

    def in_hbm(array):
        return pltpu.with_memory_space_constraint(array, pltpu.HBM)

    vmem = pl.BlockSpec(memory_space=pltpu.VMEM)
    hbm = pl.BlockSpec(memory_space=pltpu.HBM)
    edge = pltpu.VMEM((2, fields, STEPS, columns), f32)
    dma = pltpu.SemaphoreType.DMA
    increment, packed = pl.pallas_call(
        functools.partial(kernel, groups, bands),
        out_shape=(
            jax.ShapeDtypeStruct((1, fields, rows, columns), f32),
            jax.ShapeDtypeStruct((1, LANES), f32),
        ),
        in_specs=[hbm, hbm, hbm, pl.BlockSpec(memory_space=pltpu.SMEM), hbm, hbm, hbm],
        out_specs=(vmem, vmem),
        scratch_shapes=[
            pltpu.VMEM(sketch.shape, sketch.dtype),
            pltpu.VMEM(test_sketch.shape, test_sketch.dtype),
            pltpu.VMEM((rank, fields, 2 * STEPS, columns), sketch.dtype),
            pltpu.VMEM(sketch.shape, f32),
            pltpu.VMEM(test_sketch.shape, f32),
            pltpu.VMEM((rank, fields, 2 * STEPS, columns), f32),
            pltpu.VMEM((fields, rank * 2 * STEPS, columns), sketch.dtype),
            pltpu.VMEM(checkpoints.shape, checkpoints.dtype),
            pltpu.VMEM(station_row.shape, station_row.dtype),
            pltpu.VMEM(station_column.shape, station_column.dtype),
            pltpu.VMEM(station_value.shape, station_value.dtype),
            pltpu.VMEM((fields, span, columns), f32),
            pltpu.VMEM((fields, span, columns), f32),
            pltpu.VMEM((fields, span, columns), f32),
            pltpu.VMEM((fields, rows, columns), f32),
            pltpu.VMEM((fields, 2 * STEPS, columns), f32),
            pltpu.VMEM((rank, LANES), f32),
            pltpu.VMEM((rank, LANES), f32),
            edge,
            edge,
            edge,
            edge,
            edge,
            edge,
            pltpu.VMEM((1, LANES), f32),
            pltpu.VMEM((bands, 1, LANES), f32),
            pltpu.VMEM((bands, 1, LANES), f32),
            pltpu.VMEM((1, LANES), f32),
            pltpu.VMEM((bands, 1, LANES), f32),
            pltpu.VMEM((1, LANES), f32),
            pltpu.VMEM((groups, 1, LANES), f32),
            pltpu.VMEM((1, 1), f32),
            dma((8,)),
            dma((2,)),
            dma((2,)),
            dma((1,)),
            dma((1,)),
            dma((1,)),
            dma((1,)),
            dma((1,)),
            dma((1,)),
            dma((1,)),
            dma((1,)),
            dma((1,)),
            dma((1,)),
            dma((1,)),
            dma((1,)),
            dma((1,)),
            dma((1,)),
        ],
        compiler_params=pltpu.CompilerParams(
            collective_id=0,
            has_side_effects=True,
            vmem_limit_bytes=48 * 1024 * 1024,
        ),
    )(
        in_hbm(sketch),
        in_hbm(test_sketch),
        in_hbm(checkpoints),
        checkpoint_step,
        in_hbm(station_row),
        in_hbm(station_column),
        in_hbm(station_value),
    )
    keep = lax.broadcasted_iota(jnp.int32, packed.shape, 1) == rank
    return increment, packed[:, :rank], jnp.sum(jnp.where(keep, packed, 0.0))


def solution(mesh):
    placed = (
        P("tm", None, "lat", None),
        P("tm", None, "lat", None),
        P("tm", None, "lat", None),
        P("tm"),
        P("tm", "lat"),
        P("tm", "lat"),
        P("tm", "lat"),
    )
    return jax.shard_map(
        functools.partial(body, mesh.shape["tm"], mesh.shape["lat"]),
        mesh=mesh,
        in_specs=placed,
        out_specs=(P("tm", None, "lat", None), P("tm", None), P()),
        check_vma=False,
    )
```
